128 devices in a mesh: gx: 8 (over y, x_lo), gy: 16 (over x_hi, z, core).
Axes of the slice: x: 4 (x_hi: 2, x_lo: 2; x = x_hi * 2 + x_lo), y: 4, z: 4, core: 2. Of those that a mesh axis runs over, the one named last changes fastest.
Arguments:
- right_side: float32 [512, 512, 256], P('gx', 'gy'), may hold values from -45 to 45
- block_inverse: float32 [1, 256, 256], replicated, may hold values from -1 to 2
- basis_left: float32 [2, 1, 32, 256], replicated, may hold values from -0.25 to 0.25
- basis_right: float32 [2, 1, 32, 256], replicated, may hold values from -0.25 to 0.25
- ranks: int32 [2, 1, 512, 512], replicated, may hold values from 1 to 32
Outputs:
- solution_field: float32 [512, 512, 256], P('gx', 'gy')
- true_gap: float32 [512, 512, 256], P('gx', 'gy')
- preconditioned: float32 [512, 512, 256], P('gx', 'gy')
The draws below stay inside these ranges and needn't reach their ends.
All inputs are finite; a program needn't handle non-finite values.
Results may differ from the reference program's by a relative error of at most 0.0003.
Values sent between devices are 32-bit elements; how exact they have to be, the bound alone decides.
A program may use at most 64 MiB of HBM per device.

```python
import math
import jax
import jax.numpy as jnp
from jax import lax

NZ = 256
BLOCK = 256
RANK = 32
ITERS = 2
NZB = 1
NX = 512
NY = 512


def draw_right_side(key, part):
    first = jax.random.fold_in(jax.random.fold_in(key, 11), 0)
    along_x = (jnp.arange(NX, dtype=jnp.float32) / NX)[:, None, None]
    along_y = (jnp.arange(NY, dtype=jnp.float32) / NY)[None, :, None]
    scales = 3.0 ** along_x * 3.0 ** along_y
    rough = jax.random.truncated_normal(first, -5.0, 5.0, (NX, NY, NZ), jnp.float32)
    return rough * scales


def draw_block_inverse(key, part):
    inner = jax.random.fold_in(key, 23)
    sigma = 0.2 / math.sqrt(BLOCK)
    noise = jax.random.normal(inner, (NZB, BLOCK, BLOCK), jnp.float32)
    symmetric = (noise + jnp.swapaxes(noise, 1, 2)) * (sigma / math.sqrt(2.0))
    return jnp.eye(BLOCK, dtype=jnp.float32)[None, :, :] + symmetric


def with_ends(entries, rng, least, largest):
    longest = entries.shape.index(max(entries.shape))
    spots = []
    for shift in (0, 1):
        where = [jax.random.randint(jax.random.fold_in(rng, axis), (), 0, length) for axis, length in enumerate(entries.shape)]
        where[longest] = (where[longest] + shift) % entries.shape[longest]
        spots.append(tuple(where))
    return entries.at[spots[0]].set(least).at[spots[1]].set(largest)


def gaussian(rng, shape, scale, reach, kind=jnp.bfloat16):
    return jnp.clip(scale * jax.random.normal(rng, shape, jnp.float32), -reach, reach).astype(kind)


def setup_inputs(seed: int = 0) -> dict:
    arg_keys = jax.random.split(jax.random.key(seed), 6)
    right_side = draw_right_side(jax.random.fold_in(arg_keys[5], 71), 0)
    block_inverse = draw_block_inverse(jax.random.fold_in(arg_keys[5], 71), 0)
    basis_left = gaussian(arg_keys[2], (2, NZB, RANK, BLOCK), (0.3 / BLOCK ** 0.5), 0.25, jnp.float32)
    basis_right = gaussian(arg_keys[3], (2, NZB, RANK, BLOCK), (0.3 / BLOCK ** 0.5), 0.25, jnp.float32)
    ranks = with_ends(jax.random.randint(arg_keys[4], (2, NZB, NX, NY), 1, RANK + 1), jax.random.fold_in(arg_keys[4], 1), 1, RANK).astype(jnp.int32)
    return dict(right_side=right_side, block_inverse=block_inverse, basis_left=basis_left, basis_right=basis_right, ranks=ranks)


mass_shift = 0.05


def operate(field):
    beside = jnp.roll(field, 1, 0) + jnp.roll(field, -1, 0)
    beside = beside + jnp.roll(field, 1, 1) + jnp.roll(field, -1, 1)
    beside = beside + jnp.roll(field, 1, 2) + jnp.roll(field, -1, 2)
    return (6.0 + mass_shift) * field - beside


def couple_term(source, factor_in, factor_out, limits, levels):
    coef = jnp.einsum('xybc,bkc->xybk', source, factor_in, precision=lax.Precision.HIGHEST)
    keep = levels[None, None, None, :] < jnp.transpose(limits, (1, 2, 0))[..., None]
    coef = jnp.where(keep, coef, jnp.zeros_like(coef))
    return jnp.einsum('xybk,bki->xybi', coef, factor_out, precision=lax.Precision.HIGHEST)


def precondition(residual, block_inverse, basis_left, basis_right, ranks):
    nx, ny, nz = residual.shape
    nzb = block_inverse.shape[0]
    blk = block_inverse.shape[1]
    rank = basis_left.shape[2]
    blocks = residual.reshape(nx, ny, nzb, blk)
    total = jnp.einsum('xybc,bic->xybi', blocks, block_inverse, precision=lax.Precision.HIGHEST)
    levels = jnp.arange(rank, dtype=jnp.int32)
    for along in range(2):
        ahead = jnp.roll(blocks, -1, along)
        total = total + couple_term(ahead, basis_right[along], basis_left[along], ranks[along], levels)
        behind = jnp.roll(blocks, 1, along)
        limits = jnp.roll(ranks[along], 1, along + 1)
        total = total + couple_term(behind, basis_left[along], basis_right[along], limits, levels)
    return total.reshape(nx, ny, nz)


def reference(right_side, block_inverse, basis_left, basis_right, ranks):
    solution_field = jnp.zeros_like(right_side)
    residual = right_side
    precond = precondition(residual, block_inverse, basis_left, basis_right, ranks)
    direction = precond
    rz_now = jnp.sum(residual * precond)
    for step in range(ITERS):
        image = operate(direction)
        alpha = rz_now / jnp.sum(direction * image)
        solution_field = solution_field + alpha * direction
        residual = residual - alpha * image
        precond = precondition(residual, block_inverse, basis_left, basis_right, ranks)
        if step + 1 < ITERS:
            rz_next = jnp.sum(residual * precond)
            direction = precond + (rz_next / rz_now) * direction
            rz_now = rz_next
    true_gap = right_side - operate(solution_field)
    return solution_field, true_gap, precond
```

```python
import functools

import jax
import jax.numpy as jnp
from jax import lax
from jax.experimental import pallas as pl
from jax.experimental.pallas import tpu as pltpu
from jax.sharding import PartitionSpec as P

F32 = jnp.float32
BF16 = jnp.bfloat16
MESH = pl.DeviceIdType.MESH

mass_shift = 0.05

S_BU0, S_U0V0, S_BU1, S_V0U1, S_U1V1 = range(5)


def halves(value):
    high = value.astype(BF16)
    return high, (value - high.astype(F32)).astype(BF16)


def dot(a, b):
    return lax.dot_general(a, b, (((1,), (0,)), ((), ())), preferred_element_type=F32)


def fold(value):
    rows, width = value.shape
    return jnp.sum(value.reshape(rows // 8, 8, width), axis=0)


def kernel(
    devs, b_any, binv_any, left_any, right_any, ranks_any,
    x_out, gap_out, z_out,
    b, binv, bases, tiles, prev, wide, wb, wc, wd, picks, mask, split, dsplit,
    u0, u1, u2, v0, v1, c0, c1, c2,
    send_c, recv_c, send_u, recv_u, part, got_y, got_x,
    load_sem, send_sem, recv_sem, rsend_sem, rrecv_sem,
):
    ndx, ndy = devs
    nx, ny, nz = b.shape
    gx = lax.axis_index("gx")
    gy = lax.axis_index("gy")
    east, west = lax.rem(gx + 1, ndx), lax.rem(gx + ndx - 1, ndx)
    north, south = lax.rem(gy + 1, ndy), lax.rem(gy + ndy - 1, ndy)

    barrier = pltpu.get_barrier_semaphore()
    for k in range(1, ndy):
        pl.semaphore_signal(barrier, 1, device_id=(gx, lax.rem(gy + k, ndy)), device_id_type=MESH)
    for k in range(1, ndx):
        pl.semaphore_signal(barrier, 1, device_id=(lax.rem(gx + k, ndx), gy), device_id_type=MESH)

    per_tile = 128 // ny
    col = pl.multiple_of(gy // per_tile * 128, 128)
    col_back = pl.multiple_of(south // per_tile * 128, 128)
    row = pl.multiple_of(gx * nx, 8)
    row_back = pl.multiple_of(west * nx + nx - 8, 8)
    loads = [
        pltpu.make_async_copy(binv_any.at[0], binv, load_sem.at[0]),
        pltpu.make_async_copy(right_any.at[0, 0], bases.at[0], load_sem.at[1]),
        pltpu.make_async_copy(left_any.at[0, 0], bases.at[1], load_sem.at[2]),
        pltpu.make_async_copy(right_any.at[1, 0], bases.at[2], load_sem.at[3]),
        pltpu.make_async_copy(left_any.at[1, 0], bases.at[3], load_sem.at[4]),
        pltpu.make_async_copy(ranks_any.at[0, 0, pl.ds(row, nx), pl.ds(col, 128)], tiles.at[0], load_sem.at[5]),
        pltpu.make_async_copy(ranks_any.at[1, 0, pl.ds(row, nx), pl.ds(col, 128)], tiles.at[1], load_sem.at[6]),
        pltpu.make_async_copy(ranks_any.at[1, 0, pl.ds(row, nx), pl.ds(col_back, 128)], tiles.at[2], load_sem.at[7]),
        pltpu.make_async_copy(ranks_any.at[0, 0, pl.ds(row_back, 8), pl.ds(col, 128)], prev, load_sem.at[8]),
        pltpu.make_async_copy(b_any, b, load_sem.at[9]),
    ]
    for load in loads:
        load.start()

    for load in loads[:5]:
        load.wait()
    high, low = halves(binv[...].T)
    wb[0:nz, :] = high
    wb[nz : 2 * nz, :] = high
    wb[2 * nz : 3 * nz, :] = low
    factors = bases[...].reshape(4 * 32, nz)
    high, low = halves(factors.T)
    wc[0:nz, 0:128] = high
    wc[0:nz, 128:256] = low
    wc[nz : 2 * nz, 0:128] = high
    wc[nz : 2 * nz, 128:256] = jnp.zeros((nz, 128), BF16)
    swapped = jnp.concatenate([bases[1], bases[0], bases[3], bases[2]], axis=0)
    high, low = halves(swapped)
    wd[0:128, :] = high
    wd[128:256, :] = high
    wd[256:384, :] = low

    for load in loads[5:9]:
        load.wait()
    lane = lax.broadcasted_iota(jnp.int32, (nx, 128), 1)
    line = lax.broadcasted_iota(jnp.int32, (nx, 128), 0)
    shift = lax.rem(gy, per_tile) * ny
    turned = lambda value, s: pltpu.roll(value, lax.rem(128 + s - shift, 128), 1)
    first, second, second_back = (tiles[k].astype(F32) for k in range(3))
    last = jnp.broadcast_to(prev[...].astype(F32)[7:8, :], (nx, 128))
    before = jnp.where(line == 0, last, pltpu.roll(first, 1, 0))
    seg0 = turned(first, 0)
    seg1 = turned(before, 32)
    seg2 = turned(second, 64)
    seg3 = jnp.where(lane == 96, turned(second_back, 97), turned(second, 97))
    wide[...] = jnp.where(lane < 32, seg0, jnp.where(lane < 64, seg1, jnp.where(lane < 96, seg2, seg3)))
    own = lax.rem(lax.broadcasted_iota(jnp.int32, (ny, 128), 1), 32) == lax.broadcasted_iota(jnp.int32, (ny, 128), 0)
    spread = (
        lax.broadcasted_iota(jnp.int32, (128, 128), 0) // 32 == lax.broadcasted_iota(jnp.int32, (128, 128), 1) // 32
    ).astype(F32).astype(BF16)

    def place(i, _):
        line_ranks = jnp.broadcast_to(wide[pl.ds(i, 1), :], (ny, 128))
        picks[pl.ds(pl.multiple_of(i * ny, ny), ny), :] = jnp.where(own, line_ranks, 0.0).astype(BF16)
        return 0

    lax.fori_loop(0, nx, place, 0, unroll=4)
    step = 16
    rows = step * ny
    level = lax.rem(lax.broadcasted_iota(jnp.int32, (rows, 128), 1), 32).astype(F32)

    def fill_mask(i, _):
        here = pl.ds(pl.multiple_of(i * rows, rows), rows)
        mask[here, :] = jnp.where(level < dot(picks[here, :], spread), 1.0, 0.0)
        return 0

    lax.fori_loop(0, nx // step, fill_mask, 0)

    def cells(x):
        return pl.ds(pl.multiple_of((x + 1) * ny, ny), ny)

    def coefs(c, send):
        def body(i, _):
            here = pl.ds(pl.multiple_of(i * rows, rows), rows)
            both = dot(split[here, :], wc[...])
            both = both[:, :128] + both[:, 128:]
            c[pl.ds(pl.multiple_of(i * rows + ny, ny), rows), :] = both
            first = [both[j * ny : j * ny + 1, :] for j in range(step)]
            last = [both[(j + 1) * ny - 1 : (j + 1) * ny, :] for j in range(step)]
            ends(send, i, first, last)
            return 0

        lax.fori_loop(0, nx // step, body, 0)

    def exchange(k, field, send, recv):
        plan = (
            (field.at[pl.ds(ny, ny), :], field.at[pl.ds((nx + 1) * ny, ny), :], (west, gy)),
            (field.at[pl.ds(nx * ny, ny), :], field.at[pl.ds(0, ny), :], (east, gy)),
            (send.at[0], recv.at[0], (gx, south)),
            (send.at[1], recv.at[1], (gx, north)),
        )
        copies = [
            pltpu.make_async_remote_copy(
                src_ref=src, dst_ref=dst, send_sem=send_sem.at[k, n], recv_sem=recv_sem.at[k, n],
                device_id=to, device_id_type=MESH,
            )
            for n, (src, dst, to) in enumerate(plan)
        ]
        for copy in copies:
            copy.start()
        return copies

    def arrive(copies):
        for copy in copies:
            copy.wait()

    def ends(send, i, first, last):
        here = pl.ds(pl.multiple_of(i * step, step), step)
        send[0, here, :] = jnp.concatenate(first, axis=0)
        send[1, here, :] = jnp.concatenate(last, axis=0)

    def shifted(here, recv, x):
        line = lax.broadcasted_iota(jnp.int32, here.shape, 0)
        after = jnp.broadcast_to(recv[0, pl.ds(x, 1), :], here.shape)
        before = jnp.broadcast_to(recv[1, pl.ds(x, 1), :], here.shape)
        return (
            jnp.where(line == ny - 1, after, pltpu.roll(here, ny - 1, 0)),
            jnp.where(line == 0, before, pltpu.roll(here, 1, 0)),
        )

    def diagonal(write):
        def body(i, _):
            here = pl.ds(pl.multiple_of(i * rows, rows), rows)
            value = split[here, :]
            write(i, dot(jnp.concatenate([value, value[:, :nz]], axis=1), wb[...]))
            return 0

        lax.fori_loop(0, nx // step, body, 0)

    seg = lax.broadcasted_iota(jnp.int32, (ny, 128), 1) // 32

    def couple(c, recv, start, finish):
        def body(i, carry):
            for j in range(step):
                x = i * step + j
                after, before = shifted(c[cells(x), :], recv, x)
                coef = jnp.where(
                    seg == 0, c[cells(x + 1), :], jnp.where(seg == 1, c[cells(x - 1), :], jnp.where(seg == 2, after, before))
                )
                coef = coef * mask[pl.ds(pl.multiple_of(x * ny, ny), ny), :]
                high, low = halves(coef)
                dsplit[j * ny : (j + 1) * ny, 0:128] = high
                dsplit[j * ny : (j + 1) * ny, 128:256] = low
            value = dsplit[...]
            return finish(i, dot(jnp.concatenate([value, value[:, :128]], axis=1), wd[...]), carry)

        return lax.fori_loop(0, nx // step, body, start)

    def put_padded(u):
        def write(i, value):
            u[pl.ds(pl.multiple_of(i * rows + ny, ny), rows), :] = value

        return write

    zero = jnp.zeros((8, nz), F32)

    def operate(u, recv, v, sums):
        def body(x, carry):
            here = u[cells(x), :]
            after, before = shifted(here, recv, x)
            beside = u[cells(x + 1), :] + u[cells(x - 1), :] + after + before
            beside = beside + pltpu.roll(here, 1, 1) + pltpu.roll(here, nz - 1, 1)
            value = (6.0 + mass_shift) * here - beside
            v[x] = value
            at = pl.ds(pl.multiple_of(x * ny, ny), ny)
            high, low = halves(value)
            split[at, 0:nz] = high
            split[at, nz : 2 * nz] = low
            return sums(x, here, value, carry)

        return body

    loads[9].wait()

    def first_split(x, _):
        at = pl.ds(pl.multiple_of(x * ny, ny), ny)
        high, low = halves(b[x])
        split[at, 0:nz] = high
        split[at, nz : 2 * nz] = low
        return 0

    lax.fori_loop(0, nx, first_split, 0, unroll=4)
    coefs(c0, send_c.at[0])
    pl.semaphore_wait(barrier, ndx + ndy - 2)
    copies = exchange(0, c0, send_c.at[0], recv_c.at[0])
    diagonal(put_padded(u0))
    arrive(copies)

    def finish0(i, value, carry):
        first, last = [], []
        for j in range(step):
            x = i * step + j
            total = u0[cells(x), :] + value[j * ny : (j + 1) * ny, :]
            u0[cells(x), :] = total
            first.append(total[:1])
            last.append(total[ny - 1 :])
            carry = carry + fold(total * b[x])
        ends(send_u.at[0], i, first, last)
        return carry

    bu0 = couple(c0, recv_c.at[0], zero, finish0)

    copies = exchange(1, u0, send_u.at[0], recv_u.at[0])
    arrive(copies)
    body = operate(u0, recv_u.at[0], v0, lambda x, here, value, carry: carry + fold(here * value))
    u0v0 = lax.fori_loop(0, nx, body, zero, unroll=2)

    coefs(c1, send_c.at[1])
    copies = exchange(2, c1, send_c.at[1], recv_c.at[1])
    diagonal(put_padded(u1))
    arrive(copies)

    def finish1(i, value, carry):
        one, two = carry
        first, last = [], []
        for j in range(step):
            x = i * step + j
            total = u1[cells(x), :] + value[j * ny : (j + 1) * ny, :]
            u1[cells(x), :] = total
            first.append(total[:1])
            last.append(total[ny - 1 :])
            one = one + fold(total * b[x])
            two = two + fold(total * v0[x])
        ends(send_u.at[1], i, first, last)
        return one, two

    bu1, v0u1 = couple(c1, recv_c.at[1], (zero, zero), finish1)

    copies = exchange(3, u1, send_u.at[1], recv_u.at[1])
    arrive(copies)
    body = operate(u1, recv_u.at[1], v1, lambda x, here, value, carry: carry + fold(here * value))
    u1v1 = lax.fori_loop(0, nx, body, zero, unroll=2)

    def lines(value):
        value = value[:, :128] + value[:, 128:]
        return jnp.sum(value, axis=0, keepdims=True)

    partial = jnp.concatenate(
        [lines(s) for s in (bu0, u0v0, bu1, v0u1, u1v1)] + [jnp.zeros((3, 128), F32)], axis=0
    )
    part[0] = partial
    got_y[gy] = partial
    along_y = [
        pltpu.make_async_remote_copy(
            src_ref=part.at[0], dst_ref=got_y.at[gy], send_sem=rsend_sem.at[0, k], recv_sem=rrecv_sem.at[0, k],
            device_id=(gx, lax.rem(gy + k, ndy)), device_id_type=MESH,
        )
        for k in range(1, ndy)
    ]
    for copy in along_y:
        copy.start()

    coefs(c2, send_c.at[2])
    copies = exchange(4, c2, send_c.at[2], recv_c.at[2])
    for copy in along_y:
        copy.wait()
    partial = jnp.sum(got_y[...], axis=0)
    part[1] = partial
    got_x[gx] = partial
    along_x = [
        pltpu.make_async_remote_copy(
            src_ref=part.at[1], dst_ref=got_x.at[gx], send_sem=rsend_sem.at[1, k], recv_sem=rrecv_sem.at[1, k],
            device_id=(lax.rem(gx + k, ndx), gy), device_id_type=MESH,
        )
        for k in range(1, ndx)
    ]
    for copy in along_x:
        copy.start()

    def write_u2(i, value):
        u2[pl.ds(pl.multiple_of(i * rows, rows), rows), :] = value

    diagonal(write_u2)
    arrive(copies)

    def finish2(i, value, carry):
        here = pl.ds(pl.multiple_of(i * rows, rows), rows)
        u2[here, :] = u2[here, :] + value
        return carry

    couple(c2, recv_c.at[2], 0, finish2)

    for copy in along_x:
        copy.wait()
    total = jnp.sum(jnp.sum(got_x[...], axis=0), axis=1, keepdims=True)
    s = [total[k : k + 1, :] for k in range(5)]

    alpha0 = s[S_BU0] / s[S_U0V0]
    rz1 = s[S_BU0] - alpha0 * (s[S_U0V0] + s[S_BU1]) + alpha0 * (alpha0 * s[S_V0U1])
    grow = 1.0 + rz1 / s[S_BU0]
    curve = grow * (grow * s[S_U0V0] - 2.0 * (alpha0 * s[S_V0U1])) + alpha0 * (alpha0 * s[S_U1V1])
    alpha1 = rz1 / curve
    on0 = alpha0 + alpha1 * grow
    on1 = -(alpha1 * alpha0)
    on0 = jnp.broadcast_to(on0, (ny, nz))
    on1 = jnp.broadcast_to(on1, (ny, nz))

    def final(x, _):
        at = pl.ds(pl.multiple_of(x * ny, ny), ny)
        f0, f1 = u0[cells(x), :], u1[cells(x), :]
        x_out[x] = on0 * f0 + on1 * f1
        gap_out[x] = b[x] - on0 * v0[x] - on1 * v1[x]
        z_out[x] = f0 - on0 * f1 - on1 * u2[at, :]
        return 0

    lax.fori_loop(0, nx, final, 0, unroll=2)


def per_device(devs, right_side, block_inverse, basis_left, basis_right, ranks):
    nx, ny, nz = right_side.shape
    ndx, ndy = devs
    lines = nx * ny
    padded = lines + 2 * ny
    out = jax.ShapeDtypeStruct(right_side.shape, F32)
    return pl.pallas_call(
        functools.partial(kernel, devs),
        out_shape=(out, out, out),
        in_specs=[pl.BlockSpec(memory_space=pl.ANY)] * 5,
        out_specs=[pl.BlockSpec(memory_space=pltpu.VMEM)] * 3,
        scratch_shapes=[
            pltpu.VMEM((nx, ny, nz), F32),
            pltpu.VMEM((nz, nz), F32),
            pltpu.VMEM((4, 32, nz), F32),
            pltpu.VMEM((3, nx, 128), jnp.int32),
            pltpu.VMEM((8, 128), jnp.int32),
            pltpu.VMEM((nx, 128), F32),
            pltpu.VMEM((3 * nz, nz), BF16),
            pltpu.VMEM((2 * nz, 256), BF16),
            pltpu.VMEM((384, nz), BF16),
            pltpu.VMEM((lines, 128), BF16),
            pltpu.VMEM((lines, 128), F32),
            pltpu.VMEM((lines, 2 * nz), BF16),
            pltpu.VMEM((16 * ny, 256), BF16),
            pltpu.VMEM((padded, nz), F32),
            pltpu.VMEM((padded, nz), F32),
            pltpu.VMEM((lines, nz), F32),
            pltpu.VMEM((nx, ny, nz), F32),
            pltpu.VMEM((nx, ny, nz), F32),
            pltpu.VMEM((padded, 128), F32),
            pltpu.VMEM((padded, 128), F32),
            pltpu.VMEM((padded, 128), F32),
            pltpu.VMEM((3, 2, nx, 128), F32),
            pltpu.VMEM((3, 2, nx, 128), F32),
            pltpu.VMEM((2, 2, nx, nz), F32),
            pltpu.VMEM((2, 2, nx, nz), F32),
            pltpu.VMEM((2, 8, 128), F32),
            pltpu.VMEM((ndy, 8, 128), F32),
            pltpu.VMEM((ndx, 8, 128), F32),
            pltpu.SemaphoreType.DMA((10,)),
            pltpu.SemaphoreType.DMA((5, 4)),
            pltpu.SemaphoreType.DMA((5, 4)),
            pltpu.SemaphoreType.DMA((2, ndy)),
            pltpu.SemaphoreType.DMA((2, ndy)),
        ],
        compiler_params=pltpu.CompilerParams(
            collective_id=0, has_side_effects=True, vmem_limit_bytes=48 * 1024 * 1024
        ),
    )(right_side, block_inverse, basis_left, basis_right, ranks)


def solution(mesh):
    devs = (mesh.shape["gx"], mesh.shape["gy"])
    return jax.shard_map(
        functools.partial(per_device, devs),
        mesh=mesh,
        in_specs=(P("gx", "gy", None), P(), P(), P(), P()),
        out_specs=(P("gx", "gy", None),) * 3,
        check_vma=False,
    )
```

```python
import functools

import jax
import jax.numpy as jnp
from jax import lax
from jax.experimental import pallas as pl
from jax.experimental.pallas import tpu as pltpu
from jax.sharding import PartitionSpec as P

F32 = jnp.float32
BF16 = jnp.bfloat16
MESH = pl.DeviceIdType.MESH

mass_shift = 0.05

S_BU0, S_U0V0, S_BU1, S_V0U1, S_U1V1 = range(5)


def halves(value):
    high = value.astype(BF16)
    return high, (value - high.astype(F32)).astype(BF16)


def dot(a, b):
    return lax.dot_general(a, b, (((1,), (0,)), ((), ())), preferred_element_type=F32)


def fold(value):
    rows, width = value.shape
    return jnp.sum(value.reshape(rows // 8, 8, width), axis=0)


def kernel(
    devs, b_any, binv_any, left_any, right_any, ranks_any,
    b, u0, u1, u2, v0, v1, scale,
    binv, bases, tiles, prev, wide, wb, wc, wd, picks, mask, split, dsplit,
    c0, c1, c2,
    send_c, recv_c, send_u, recv_u, part, got_y, got_x,
    load_sem, xsend_sem, xrecv_sem, ysend_sem, yrecv_sem, rsend_sem, rrecv_sem,
):
    ndx, ndy = devs
    nx, ny, nz = b.shape
    gx = lax.axis_index("gx")
    gy = lax.axis_index("gy")
    east, west = lax.rem(gx + 1, ndx), lax.rem(gx + ndx - 1, ndx)
    north, south = lax.rem(gy + 1, ndy), lax.rem(gy + ndy - 1, ndy)

    barrier = pltpu.get_barrier_semaphore()
    for k in range(1, ndy):
        pl.semaphore_signal(barrier, 1, device_id=(gx, lax.rem(gy + k, ndy)), device_id_type=MESH)
    for k in range(1, ndx):
        pl.semaphore_signal(barrier, 1, device_id=(lax.rem(gx + k, ndx), gy), device_id_type=MESH)

    per_tile = 128 // ny
    col = pl.multiple_of(gy // per_tile * 128, 128)
    col_back = pl.multiple_of(south // per_tile * 128, 128)
    row = pl.multiple_of(gx * nx, 8)
    row_back = pl.multiple_of(west * nx + nx - 8, 8)
    loads = [
        pltpu.make_async_copy(binv_any.at[0], binv, load_sem.at[0]),
        pltpu.make_async_copy(right_any.at[0, 0], bases.at[0], load_sem.at[1]),
        pltpu.make_async_copy(left_any.at[0, 0], bases.at[1], load_sem.at[2]),
        pltpu.make_async_copy(right_any.at[1, 0], bases.at[2], load_sem.at[3]),
        pltpu.make_async_copy(left_any.at[1, 0], bases.at[3], load_sem.at[4]),
        pltpu.make_async_copy(ranks_any.at[0, 0, pl.ds(row, nx), pl.ds(col, 128)], tiles.at[0], load_sem.at[5]),
        pltpu.make_async_copy(ranks_any.at[1, 0, pl.ds(row, nx), pl.ds(col, 128)], tiles.at[1], load_sem.at[6]),
        pltpu.make_async_copy(ranks_any.at[1, 0, pl.ds(row, nx), pl.ds(col_back, 128)], tiles.at[2], load_sem.at[7]),
        pltpu.make_async_copy(ranks_any.at[0, 0, pl.ds(row_back, 8), pl.ds(col, 128)], prev, load_sem.at[8]),
        pltpu.make_async_copy(b_any, b, load_sem.at[9]),
    ]
    for load in loads:
        load.start()

    for load in loads[:5]:
        load.wait()
    high, low = halves(binv[...].T)
    wb[0:nz, :] = high
    wb[nz : 2 * nz, :] = high
    wb[2 * nz : 3 * nz, :] = low
    factors = bases[...].reshape(4 * 32, nz)
    high, low = halves(factors.T)
    wc[0:nz, 0:128] = high
    wc[0:nz, 128:256] = low
    wc[nz : 2 * nz, 0:128] = high
    wc[nz : 2 * nz, 128:256] = jnp.zeros((nz, 128), BF16)
    swapped = jnp.concatenate([bases[1], bases[0], bases[3], bases[2]], axis=0)
    high, low = halves(swapped)
    wd[0:128, :] = high
    wd[128:256, :] = high
    wd[256:384, :] = low

    for load in loads[5:9]:
        load.wait()
    lane = lax.broadcasted_iota(jnp.int32, (nx, 128), 1)
    line = lax.broadcasted_iota(jnp.int32, (nx, 128), 0)
    shift = lax.rem(gy, per_tile) * ny
    turned = lambda value, s: pltpu.roll(value, lax.rem(128 + s - shift, 128), 1)
    first, second, second_back = (tiles[k].astype(F32) for k in range(3))
    last = jnp.broadcast_to(prev[...].astype(F32)[7:8, :], (nx, 128))
    before = jnp.where(line == 0, last, pltpu.roll(first, 1, 0))
    seg0 = turned(first, 0)
    seg1 = turned(before, 32)
    seg2 = turned(second, 64)
    seg3 = jnp.where(lane == 96, turned(second_back, 97), turned(second, 97))
    wide[...] = jnp.where(lane < 32, seg0, jnp.where(lane < 64, seg1, jnp.where(lane < 96, seg2, seg3)))
    own = lax.rem(lax.broadcasted_iota(jnp.int32, (ny, 128), 1), 32) == lax.broadcasted_iota(jnp.int32, (ny, 128), 0)
    spread = (
        lax.broadcasted_iota(jnp.int32, (128, 128), 0) // 32 == lax.broadcasted_iota(jnp.int32, (128, 128), 1) // 32
    ).astype(F32).astype(BF16)

    def place(i, _):
        line_ranks = jnp.broadcast_to(wide[pl.ds(i, 1), :], (ny, 128))
        picks[pl.ds(pl.multiple_of(i * ny, ny), ny), :] = jnp.where(own, line_ranks, 0.0).astype(BF16)
        return 0

    lax.fori_loop(0, nx, place, 0, unroll=4)
    step = 16
    rows = step * ny
    level = lax.rem(lax.broadcasted_iota(jnp.int32, (rows, 128), 1), 32).astype(F32)

    def fill_mask(i, _):
        here = pl.ds(pl.multiple_of(i * rows, rows), rows)
        mask[here, :] = jnp.where(level < dot(picks[here, :], spread), 1.0, 0.0)
        return 0

    lax.fori_loop(0, nx // step, fill_mask, 0)

    chunks = nx // step

    def chunk(i):
        return jnp.where(i == 0, 0, jnp.where(i == 1, chunks - 1, i - 1))

    def cells(x):
        return pl.ds(pl.multiple_of((x + 1) * ny, ny), ny)

    def flat(i):
        return pl.ds(pl.multiple_of(i * rows, rows), rows)

    def inner(i):
        return pl.ds(pl.multiple_of(i * rows + ny, ny), rows)

    class Halo:
        def __init__(self, k, field, send, recv):
            self.k, self.field, self.send, self.recv = k, field, send, recv

        def x_copy(self, side):
            mine, theirs, to = ((ny, (nx + 1) * ny, west), (nx * ny, 0, east))[side]
            return pltpu.make_async_remote_copy(
                src_ref=self.field.at[pl.ds(mine, ny), :], dst_ref=self.field.at[pl.ds(theirs, ny), :],
                send_sem=xsend_sem.at[self.k, side], recv_sem=xrecv_sem.at[self.k, side],
                device_id=(to, gy), device_id_type=MESH,
            )

        def y_copy(self, side, i):
            here = pl.ds(pl.multiple_of(i * step, step), step)
            return pltpu.make_async_remote_copy(
                src_ref=self.send.at[side, here, :], dst_ref=self.recv.at[side, here, :],
                send_sem=ysend_sem.at[self.k, side, i], recv_sem=yrecv_sem.at[self.k, side, i],
                device_id=(gx, (south, north)[side]), device_id_type=MESH,
            )

        def store_ends(self, i, first, last):
            here = pl.ds(pl.multiple_of(i * step, step), step)
            self.send[0, here, :] = jnp.concatenate(first, axis=0)
            self.send[1, here, :] = jnp.concatenate(last, axis=0)

        def start(self, turn, i):
            @pl.when(turn == 0)
            def _():
                self.x_copy(0).start()

            @pl.when(turn == 1)
            def _():
                self.x_copy(1).start()

            for side in (0, 1):
                self.y_copy(side, i).start()

        def arrive(self, turn, i):
            @pl.when(turn == 0)
            def _():
                self.x_copy(1).wait_recv()

            @pl.when(turn == 1)
            def _():
                self.x_copy(0).wait_recv()

            for side in (0, 1):
                self.y_copy(side, i).wait_recv()

        def drain(self):
            for side in (0, 1):
                self.x_copy(side).wait_send()
                for i in range(chunks):
                    self.y_copy(side, i).wait_send()

    cs = [Halo(k, c, send_c.at[k], recv_c.at[k]) for k, c in enumerate((c0, c1, c2))]
    us = [Halo(3 + k, u, send_u.at[k], recv_u.at[k]) for k, u in enumerate((u0, u1))]

    def coefs(halo, i):
        both = dot(split[flat(i), :], wc[...])
        both = both[:, :128] + both[:, 128:]
        halo.field[inner(i), :] = both
        halo.store_ends(
            i,
            [both[j * ny : j * ny + 1, :] for j in range(step)],
            [both[(j + 1) * ny - 1 : (j + 1) * ny, :] for j in range(step)],
        )

    def shifted(here, recv, x):
        line = lax.broadcasted_iota(jnp.int32, here.shape, 0)
        after = jnp.broadcast_to(recv[0, pl.ds(x, 1), :], here.shape)
        before = jnp.broadcast_to(recv[1, pl.ds(x, 1), :], here.shape)
        return (
            jnp.where(line == ny - 1, after, pltpu.roll(here, ny - 1, 0)),
            jnp.where(line == 0, before, pltpu.roll(here, 1, 0)),
        )

    def diagonal(out, place):
        def body(i, _):
            value = split[flat(i), :]
            out[place(i), :] = dot(jnp.concatenate([value, value[:, :nz]], axis=1), wb[...])
            return 0

        lax.fori_loop(0, chunks, body, 0)

    seg = lax.broadcasted_iota(jnp.int32, (ny, 128), 1) // 32

    def couple(halo, start, finish):
        c, recv = halo.field, halo.recv

        def body(turn, carry):
            i = chunk(turn)
            halo.arrive(turn, i)
            for j in range(step):
                x = i * step + j
                after, before = shifted(c[cells(x), :], recv, x)
                coef = jnp.where(
                    seg == 0, c[cells(x + 1), :], jnp.where(seg == 1, c[cells(x - 1), :], jnp.where(seg == 2, after, before))
                )
                coef = coef * mask[pl.ds(pl.multiple_of(x * ny, ny), ny), :]
                high, low = halves(coef)
                dsplit[j * ny : (j + 1) * ny, 0:128] = high
                dsplit[j * ny : (j + 1) * ny, 128:256] = low
            value = dsplit[...]
            return finish(turn, i, dot(jnp.concatenate([value, value[:, :128]], axis=1), wd[...]), carry)

        return lax.fori_loop(0, chunks, body, start)

    zero = jnp.zeros((8, nz), F32)

    def finish_field(halo, sums):
        u = halo.field

        def finish(turn, i, value, carry):
            first, last = [], []
            for j in range(step):
                x = i * step + j
                total = u[cells(x), :] + value[j * ny : (j + 1) * ny, :]
                u[cells(x), :] = total
                first.append(total[:1])
                last.append(total[ny - 1 :])
                carry = sums(x, total, carry)
            halo.store_ends(i, first, last)
            halo.start(turn, i)
            return carry

        return finish

    def operate(halo, v, next_halo):
        u, recv = halo.field, halo.recv

        def body(turn, carry):
            i = chunk(turn)
            halo.arrive(turn, i)

            def line(j, carry):
                x = i * step + j
                here = u[cells(x), :]
                after, before = shifted(here, recv, x)
                beside = u[cells(x + 1), :] + u[cells(x - 1), :] + after + before
                beside = beside + pltpu.roll(here, 1, 1) + pltpu.roll(here, nz - 1, 1)
                value = (6.0 + mass_shift) * here - beside
                v[x] = value
                at = pl.ds(pl.multiple_of(x * ny, ny), ny)
                high, low = halves(value)
                split[at, 0:nz] = high
                split[at, nz : 2 * nz] = low
                return carry + fold(here * value)

            carry = lax.fori_loop(0, step, line, carry, unroll=4)
            coefs(next_halo, i)
            next_halo.start(turn, i)
            return carry

        return lax.fori_loop(0, chunks, body, zero)

    loads[9].wait()

    def first_split(x, _):
        at = pl.ds(pl.multiple_of(x * ny, ny), ny)
        high, low = halves(b[x])
        split[at, 0:nz] = high
        split[at, nz : 2 * nz] = low
        return 0

    lax.fori_loop(0, nx, first_split, 0, unroll=4)

    def first_coefs(i, _):
        coefs(cs[0], i)
        return 0

    lax.fori_loop(0, chunks, first_coefs, 0)
    diagonal(u0, inner)
    pl.semaphore_wait(barrier, ndx + ndy - 2)

    def first_start(turn, _):
        cs[0].start(turn, chunk(turn))
        return 0

    lax.fori_loop(0, chunks, first_start, 0)
    bu0 = couple(cs[0], zero, finish_field(us[0], lambda x, total, carry: carry + fold(total * b[x])))

    u0v0 = operate(us[0], v0, cs[1])

    diagonal(u1, inner)
    bu1, v0u1 = couple(
        cs[1],
        (zero, zero),
        finish_field(us[1], lambda x, total, carry: (carry[0] + fold(total * b[x]), carry[1] + fold(total * v0[x]))),
    )

    u1v1 = operate(us[1], v1, cs[2])

    def lines(value):
        value = value[:, :128] + value[:, 128:]
        return jnp.sum(value, axis=0, keepdims=True)

    partial = jnp.concatenate(
        [lines(s) for s in (bu0, u0v0, bu1, v0u1, u1v1)] + [jnp.zeros((3, 128), F32)], axis=0
    )
    part[0] = partial
    got_y[gy] = partial
    along_y = [
        pltpu.make_async_remote_copy(
            src_ref=part.at[0], dst_ref=got_y.at[gy], send_sem=rsend_sem.at[0, k], recv_sem=rrecv_sem.at[0, k],
            device_id=(gx, lax.rem(gy + k, ndy)), device_id_type=MESH,
        )
        for k in range(1, ndy)
    ]
    for copy in along_y:
        copy.start()

    diagonal(u2, flat)
    for copy in along_y:
        copy.wait()
    partial = jnp.sum(got_y[...], axis=0)
    part[1] = partial
    got_x[gx] = partial
    along_x = [
        pltpu.make_async_remote_copy(
            src_ref=part.at[1], dst_ref=got_x.at[gx], send_sem=rsend_sem.at[1, k], recv_sem=rrecv_sem.at[1, k],
            device_id=(lax.rem(gx + k, ndx), gy), device_id_type=MESH,
        )
        for k in range(1, ndx)
    ]
    for copy in along_x:
        copy.start()

    def finish2(turn, i, value, carry):
        u2[flat(i), :] = u2[flat(i), :] + value
        return carry

    couple(cs[2], 0, finish2)
    for halo in cs + us:
        halo.drain()
    for copy in along_x:
        copy.wait()
    total = jnp.sum(jnp.sum(got_x[...], axis=0), axis=1, keepdims=True)
    s = [total[k : k + 1, :] for k in range(5)]

    alpha0 = s[S_BU0] / s[S_U0V0]
    rz1 = s[S_BU0] - alpha0 * (s[S_U0V0] + s[S_BU1]) + alpha0 * (alpha0 * s[S_V0U1])
    grow = 1.0 + rz1 / s[S_BU0]
    curve = grow * (grow * s[S_U0V0] - 2.0 * (alpha0 * s[S_V0U1])) + alpha0 * (alpha0 * s[S_U1V1])
    alpha1 = rz1 / curve
    on0 = alpha0 + alpha1 * grow
    on1 = -(alpha1 * alpha0)
    scale[0] = jnp.broadcast_to(on0, (8, 128))
    scale[1] = jnp.broadcast_to(on1, (8, 128))


def combine(b, u0, u1, u2, v0, v1, scale, x_any, gap_any, z_any, x_out, gap_out, z_out, sem):
    nx, ny, nz = x_out.shape
    step = 8
    on0, on1 = (jnp.concatenate([jnp.concatenate([scale[k]] * 2, axis=1)] * (ny // 8), axis=0) for k in (0, 1))

    def copies(i):
        here = pl.ds(pl.multiple_of(i * step, step), step)
        return [
            pltpu.make_async_copy(out.at[here], out_any.at[here], sem.at[n, i])
            for n, (out, out_any) in enumerate(((x_out, x_any), (z_out, z_any), (gap_out, gap_any)))
        ]

    def body(i, _):
        for j in range(step):
            x = i * step + j
            at = pl.ds(pl.multiple_of((x + 1) * ny, ny), ny)
            f0, f1 = u0[at, :], u1[at, :]
            x_out[x] = on0 * f0 + on1 * f1
            z_out[x] = f0 - on0 * f1 - on1 * u2[pl.ds(pl.multiple_of(x * ny, ny), ny), :]
            gap_out[x] = b[x] - on0 * v0[x] - on1 * v1[x]
        for copy in copies(i):
            copy.start()
        return 0

    lax.fori_loop(0, nx // step, body, 0)

    def finish(i, _):
        for copy in copies(i):
            copy.wait()
        return 0

    lax.fori_loop(0, nx // step, finish, 0)


def per_device(devs, right_side, block_inverse, basis_left, basis_right, ranks):
    nx, ny, nz = right_side.shape
    ndx, ndy = devs
    lines = nx * ny
    padded = lines + 2 * ny
    block = jax.ShapeDtypeStruct(right_side.shape, F32)
    framed = jax.ShapeDtypeStruct((padded, nz), F32)
    arrays = (right_side, block_inverse, basis_left, basis_right, ranks)
    fields = pl.pallas_call(
        functools.partial(kernel, devs),
        out_shape=(
            block, framed, framed, jax.ShapeDtypeStruct((lines, nz), F32), block, block,
            jax.ShapeDtypeStruct((2, 8, 128), F32),
        ),
        in_specs=[pl.BlockSpec(memory_space=pltpu.HBM)] * 5,
        out_specs=[pl.BlockSpec(memory_space=pltpu.VMEM)] * 7,
        scratch_shapes=[
            pltpu.VMEM((nz, nz), F32),
            pltpu.VMEM((4, 32, nz), F32),
            pltpu.VMEM((3, nx, 128), jnp.int32),
            pltpu.VMEM((8, 128), jnp.int32),
            pltpu.VMEM((nx, 128), F32),
            pltpu.VMEM((3 * nz, nz), BF16),
            pltpu.VMEM((2 * nz, 256), BF16),
            pltpu.VMEM((384, nz), BF16),
            pltpu.VMEM((lines, 128), BF16),
            pltpu.VMEM((lines, 128), F32),
            pltpu.VMEM((lines, 2 * nz), BF16),
            pltpu.VMEM((16 * ny, 256), BF16),
            pltpu.VMEM((padded, 128), F32),
            pltpu.VMEM((padded, 128), F32),
            pltpu.VMEM((padded, 128), F32),
            pltpu.VMEM((3, 2, nx, 128), F32),
            pltpu.VMEM((3, 2, nx, 128), F32),
            pltpu.VMEM((2, 2, nx, nz), F32),
            pltpu.VMEM((2, 2, nx, nz), F32),
            pltpu.VMEM((2, 8, 128), F32),
            pltpu.VMEM((ndy, 8, 128), F32),
            pltpu.VMEM((ndx, 8, 128), F32),
            pltpu.SemaphoreType.DMA((10,)),
            pltpu.SemaphoreType.DMA((5, 2)),
            pltpu.SemaphoreType.DMA((5, 2)),
            pltpu.SemaphoreType.DMA((5, 2, nx // 16)),
            pltpu.SemaphoreType.DMA((5, 2, nx // 16)),
            pltpu.SemaphoreType.DMA((2, ndy)),
            pltpu.SemaphoreType.DMA((2, ndy)),
        ],
        compiler_params=pltpu.CompilerParams(
            collective_id=0, has_side_effects=True, vmem_limit_bytes=32 * 1024 * 1024
        ),
    )(*(pltpu.with_memory_space_constraint(array, pltpu.HBM) for array in arrays))
    return pl.pallas_call(
        combine,
        out_shape=(block, block, block),
        in_specs=[pl.BlockSpec(memory_space=pltpu.VMEM)] * 7,
        out_specs=[pl.BlockSpec(memory_space=pltpu.HBM)] * 3,
        scratch_shapes=[pltpu.VMEM((nx, ny, nz), F32)] * 3 + [pltpu.SemaphoreType.DMA((3, nx // 8))],
        compiler_params=pltpu.CompilerParams(vmem_limit_bytes=32 * 1024 * 1024),
    )(*fields)


def solution(mesh):
    devs = (mesh.shape["gx"], mesh.shape["gy"])
    return jax.shard_map(
        functools.partial(per_device, devs),
        mesh=mesh,
        in_specs=(P("gx", "gy", None), P(), P(), P(), P()),
        out_specs=(P("gx", "gy", None),) * 3,
        check_vma=False,
    )
```

```python
import functools

import jax
import jax.numpy as jnp
from jax import lax
from jax.experimental import pallas as pl
from jax.experimental.pallas import tpu as pltpu
from jax.sharding import PartitionSpec as P

F32 = jnp.float32
BF16 = jnp.bfloat16
MESH = pl.DeviceIdType.MESH

mass_shift = 0.05

S_BU0, S_U0V0, S_BU1, S_V0U1, S_U1V1 = range(5)


def halves(value):
    high = value.astype(BF16)
    return high, (value - high.astype(F32)).astype(BF16)


def dot(a, b):
    return lax.dot_general(a, b, (((1,), (0,)), ((), ())), preferred_element_type=F32)


def fold(value):
    rows, width = value.shape
    return jnp.sum(value.reshape(rows // 8, 8, width), axis=0)


def kernel(
    devs, b_any, binv_any, left_any, right_any, ranks_any,
    b, u0, u1, u2, v0, v1, scale,
    binv, bases, tiles, limits, picks, wb, wc, wd, mask, edge_mask, split, dsplit, fsplit,
    c, coef_send, coef_recv, raw_send, raw_recv, corner_send, corner_recv, uy, part, got_y, got_x,
    load_sem, xsend_sem, xrecv_sem, ysend_sem, yrecv_sem, ksend_sem, krecv_sem, rsend_sem, rrecv_sem,
):
    ndx, ndy = devs
    nx, ny, nz = b.shape
    lines = nx * ny
    edge = 2 * ny + 2 * nx
    step = 16
    rows = step * ny
    chunks = nx // step
    gx = lax.axis_index("gx")
    gy = lax.axis_index("gy")
    east, west = lax.rem(gx + 1, ndx), lax.rem(gx + ndx - 1, ndx)
    north, south = lax.rem(gy + 1, ndy), lax.rem(gy + ndy - 1, ndy)
    diagonals = ((east, north), (east, south), (west, north), (west, south))

    barrier = pltpu.get_barrier_semaphore()
    for k in range(1, ndy):
        pl.semaphore_signal(barrier, 1, device_id=(gx, lax.rem(gy + k, ndy)), device_id_type=MESH)
    for k in range(1, ndx):
        pl.semaphore_signal(barrier, 1, device_id=(lax.rem(gx + k, ndx), gy), device_id_type=MESH)
    for to in diagonals:
        pl.semaphore_signal(barrier, 1, device_id=to, device_id_type=MESH)

    per_tile = 128 // ny
    tile_count = ndy // per_tile
    tile = gy // per_tile
    row_starts = (
        (0, lax.rem(gx * nx + ndx * nx - 8, ndx * nx), 8),
        (8, gx * nx, nx),
        (8 + nx, lax.rem(gx * nx + nx, ndx * nx), 8),
    )
    loads = [
        pltpu.make_async_copy(binv_any.at[0], binv, load_sem.at[0]),
        pltpu.make_async_copy(right_any.at[0, 0], bases.at[0], load_sem.at[1]),
        pltpu.make_async_copy(left_any.at[0, 0], bases.at[1], load_sem.at[2]),
        pltpu.make_async_copy(right_any.at[1, 0], bases.at[2], load_sem.at[3]),
        pltpu.make_async_copy(left_any.at[1, 0], bases.at[3], load_sem.at[4]),
        pltpu.make_async_copy(b_any, b, load_sem.at[5]),
    ]
    for e in (0, 1):
        for side in (0, 1, 2):
            col = pl.multiple_of(lax.rem(tile + side + tile_count - 1, tile_count) * 128, 128)
            for to, start, count in row_starts:
                loads.append(
                    pltpu.make_async_copy(
                        ranks_any.at[e, 0, pl.ds(pl.multiple_of(start, 8), count), pl.ds(col, 128)],
                        tiles.at[e, side, pl.ds(to, count)],
                        load_sem.at[len(loads)],
                    )
                )
    for load in loads:
        load.start()

    for k in range(3):
        c[k, 0:ny, :] = jnp.zeros((ny, 128), F32)
        c[k, (nx + 1) * ny : (nx + 2) * ny, :] = jnp.zeros((ny, 128), F32)

    for load in loads[:5]:
        load.wait()
    high, low = halves(binv[...].T)
    wb[0:nz, :] = high
    wb[nz : 2 * nz, :] = high
    wb[2 * nz : 3 * nz, :] = low
    factors = bases[...].reshape(4 * 32, nz)
    high, low = halves(factors.T)
    wc[0:nz, 0:128] = high
    wc[0:nz, 128:256] = low
    wc[nz : 2 * nz, 0:128] = high
    wc[nz : 2 * nz, 128:256] = jnp.zeros((nz, 128), BF16)
    swapped = jnp.concatenate([bases[1], bases[0], bases[3], bases[2]], axis=0)
    high, low = halves(swapped)
    wd[0:128, :] = high
    wd[128:256, :] = high
    wd[256:384, :] = low

    def cells(x):
        return pl.ds(pl.multiple_of((x + 1) * ny, ny), ny)

    def flat(i):
        return pl.ds(pl.multiple_of(i * rows, rows), rows)

    def inner(i):
        return pl.ds(pl.multiple_of(i * rows + ny, ny), rows)

    def segments(count):
        return lax.broadcasted_iota(jnp.int32, (count, 128), 1) // 32

    loads[5].wait()

    def put_split(x, value):
        at = pl.ds(pl.multiple_of(x * ny, ny), ny)
        high, low = halves(value)
        split[at, 0:nz] = high
        split[at, nz : 2 * nz] = low

    def put_ends(k, start, first, last):
        here = pl.ds(pl.multiple_of(start, 8), 8)
        raw_send[k, 0, here, :] = jnp.concatenate(first, axis=0)
        raw_send[k, 1, here, :] = jnp.concatenate(last, axis=0)

    def first_split(g, _):
        first, last = [], []
        for j in range(8):
            value = b[g * 8 + j]
            put_split(g * 8 + j, value)
            first.append(value[:1])
            last.append(value[ny - 1 :])
        put_ends(0, g * 8, first, last)
        return 0

    lax.fori_loop(0, nx // 8, first_split, 0)

    def coefs(k, i):
        both = dot(split[flat(i), :], wc[...])
        c[k, inner(i), :] = both[:, :128] + both[:, 128:]

    def pack_y(k, i):
        seg = segments(step)
        base = pl.multiple_of(i * rows + ny, ny)
        first, second = (c[k, pl.ds(base + n, step, stride=ny), :] for n in (0, 1))
        last, before = (c[k, pl.ds(base + ny - n, step, stride=ny), :] for n in (1, 2))
        coef_send[k, pl.ds(pl.multiple_of(2 * ny + i * step, step), step), :] = jnp.where(
            seg == 3, pltpu.roll(second, 32, 1), first
        )
        coef_send[k, pl.ds(pl.multiple_of(2 * ny + nx + i * step, step), step), :] = jnp.where(
            seg == 2, pltpu.roll(before, 96, 1), last
        )

    def pack_x(k, side):
        seg = segments(ny)
        x, behind, where, turn = ((0, 1, 1, 32), (nx - 1, nx - 2, 0, 96))[side]
        own = c[k, cells(x), :]
        coef_send[k, pl.ds(side * ny, ny), :] = jnp.where(seg == where, pltpu.roll(c[k, cells(behind), :], turn, 1), own)
        if k < 2:
            corner_send[k, 2 * (1 - side)] = jnp.broadcast_to(own[ny - 1 :], (8, 128))
            corner_send[k, 2 * (1 - side) + 1] = jnp.broadcast_to(own[:1], (8, 128))

    fields = (b, v0)

    def x_copies(k, side):
        to = ((west, gy), (east, gy))[side]
        mine, theirs = side * ny, (1 - side) * ny
        pairs = [(coef_send.at[k, pl.ds(mine, ny)], coef_recv.at[k, pl.ds(theirs, ny)])]
        if k < 2:
            pairs.append((fields[k].at[(0, nx - 1)[side]], raw_recv.at[k, pl.ds(theirs, ny)]))
        copies = [
            pltpu.make_async_remote_copy(
                src_ref=src, dst_ref=dst, send_sem=xsend_sem.at[k, side, n], recv_sem=xrecv_sem.at[k, side, n],
                device_id=to, device_id_type=MESH,
            )
            for n, (src, dst) in enumerate(pairs)
        ]
        if k < 2:
            for n in (2 * (1 - side), 2 * (1 - side) + 1):
                copies.append(
                    pltpu.make_async_remote_copy(
                        src_ref=corner_send.at[k, n], dst_ref=corner_recv.at[k, n],
                        send_sem=ksend_sem.at[k, n], recv_sem=krecv_sem.at[k, n],
                        device_id=diagonals[n], device_id_type=MESH,
                    )
                )
        return copies

    def y_copies(k, side, i):
        here = pl.ds(pl.multiple_of(i * step, step), step)
        there = pl.ds(pl.multiple_of(2 * ny + side * nx + i * step, step), step)
        pairs = [(coef_send.at[k, there], coef_recv.at[k, there])]
        if k < 2:
            pairs.append((raw_send.at[k, side, here], raw_recv.at[k, there]))
        return [
            pltpu.make_async_remote_copy(
                src_ref=src, dst_ref=dst, send_sem=ysend_sem.at[k, side, n, i], recv_sem=yrecv_sem.at[k, side, n, i],
                device_id=(gx, (south, north)[side]), device_id_type=MESH,
            )
            for n, (src, dst) in enumerate(pairs)
        ]

    def send_chunk(k, turn, i):
        for side in (0, 1):

            @pl.when(turn == side)
            def _():
                pack_x(k, side)
                for copy in x_copies(k, side):
                    copy.start()

        pack_y(k, i)
        for side in (0, 1):
            for copy in y_copies(k, side, i):
                copy.start()

    def all_copies(k):
        return [copy for side in (0, 1) for copy in x_copies(k, side)] + [
            copy for side in (0, 1) for i in range(chunks) for copy in y_copies(k, side, i)
        ]

    def chunk(turn):
        return jnp.where(turn == 0, 0, jnp.where(turn == 1, chunks - 1, turn - 1))

    def diagonal(out, place):
        def body(i, _):
            value = split[flat(i), :]
            out[place(i), :] = dot(jnp.concatenate([value, value[:, :nz]], axis=1), wb[...])
            return 0

        lax.fori_loop(0, chunks, body, 0)

    def couple(k, out, place):
        seg = segments(ny)
        line = lax.broadcasted_iota(jnp.int32, (ny, 128), 0)
        use_after = (seg == 2) & (line < ny - 1)
        use_before = (seg == 3) & (line > 0)

        def body(i, _):
            for j in range(step):
                x = i * step + j
                here = c[k, cells(x), :]
                coef = jnp.where(seg == 0, c[k, cells(x + 1), :], jnp.where(seg == 1, c[k, cells(x - 1), :], 0.0))
                coef = jnp.where(use_after, pltpu.roll(here, ny - 1, 0), coef)
                coef = jnp.where(use_before, pltpu.roll(here, 1, 0), coef)
                coef = coef * mask[pl.ds(pl.multiple_of(x * ny, ny), ny), :]
                high, low = halves(coef)
                dsplit[j * ny : (j + 1) * ny, 0:128] = high
                dsplit[j * ny : (j + 1) * ny, 128:256] = low
            value = dsplit[...]
            out[place(i), :] = out[place(i), :] + dot(jnp.concatenate([value, value[:, :128]], axis=1), wd[...])
            return 0

        lax.fori_loop(0, chunks, body, 0)

    def add_ends(out, at, first, last):
        line = lax.broadcasted_iota(jnp.int32, (8, nz), 0)

        def body(x, _):
            head = pl.ds(pl.multiple_of(at + x * ny, 8), 8)
            tail = pl.ds(pl.multiple_of(at + x * ny + ny - 8, 8), 8)
            more = jnp.broadcast_to(fsplit_out[pl.ds(first + x, 1), :], (8, nz))
            out[head, :] = out[head, :] + jnp.where(line == 0, more, 0.0)
            more = jnp.broadcast_to(fsplit_out[pl.ds(last + x, 1), :], (8, nz))
            out[tail, :] = out[tail, :] + jnp.where(line == 7, more, 0.0)
            return 0

        lax.fori_loop(0, nx, body, 0, unroll=8)

    fsplit_out = uy

    def put_fix(at, value):
        high, low = halves(value)
        fsplit[at : at + value.shape[0], 0:128] = high
        fsplit[at : at + value.shape[0], 128:256] = low

    def fix_own(k):
        put_fix(0, coef_recv[k] * edge_mask[...])

    def fix_halo(k):
        got = lambda at, count: coef_recv[k, at : at + count, :]
        corner = lambda n, count: jnp.broadcast_to(corner_recv[k, n][:1], (count, 128))
        ws, wn, es, en = range(4)
        seg = segments(ny)
        line = lax.broadcasted_iota(jnp.int32, (ny, 128), 0)
        for side, (lo, hi) in enumerate(((ws, wn), (es, en))):
            here = got(side * ny, ny)
            after = jnp.where(line == ny - 1, corner(hi, ny), pltpu.roll(here, ny - 1, 0))
            before = jnp.where(line == 0, corner(lo, ny), pltpu.roll(here, 1, 0))
            if side == 0:
                ahead, behind = c[k, cells(0), :], pltpu.roll(here, 32, 1)
            else:
                ahead, behind = pltpu.roll(here, 96, 1), c[k, cells(nx - 1), :]
            coef = jnp.where(seg == 0, ahead, jnp.where(seg == 1, behind, jnp.where(seg == 2, after, before)))
            put_fix(edge + side * ny, coef * mask[lines + side * ny : lines + (side + 1) * ny, :])
        seg = segments(nx)
        line = lax.broadcasted_iota(jnp.int32, (nx, 128), 0)
        for side, (lo, hi) in enumerate(((wn, en), (ws, es))):
            at = 2 * ny + side * nx
            here = got(at, nx)
            ahead = jnp.where(line == nx - 1, corner(hi, nx), pltpu.roll(here, nx - 1, 0))
            behind = jnp.where(line == 0, corner(lo, nx), pltpu.roll(here, 1, 0))
            if side == 0:
                after = pltpu.roll(here, 96, 1)
                before = c[k, pl.ds(ny + ny - 1, nx, stride=ny), :]
            else:
                after = c[k, pl.ds(ny, nx, stride=ny), :]
                before = pltpu.roll(here, 32, 1)
            coef = jnp.where(seg == 0, ahead, jnp.where(seg == 1, behind, jnp.where(seg == 2, after, before)))
            put_fix(edge + at, coef * mask[lines + at : lines + at + nx, :])

    def finish_field(k, u):
        for copy in all_copies(k):
            copy.wait_recv()
        fix_own(k)
        fix_halo(k)
        high, low = halves(raw_recv[k])
        value = fsplit[...]
        more = dot(jnp.concatenate([value, value[:, :128]], axis=1), wd[...])
        halo = more[edge:] + dot(jnp.concatenate([high, low, high], axis=1), wb[...])
        u[0:ny, :] = halo[:ny]
        u[(nx + 1) * ny : (nx + 2) * ny, :] = halo[ny : 2 * ny]
        uy[0 : 2 * nx, :] = halo[2 * ny :]
        uy[2 * nx : 4 * nx, :] = more[2 * ny : edge]
        u[cells(0), :] = u[cells(0), :] + more[:ny]
        u[cells(nx - 1), :] = u[cells(nx - 1), :] + more[ny : 2 * ny]
        add_ends(u, ny, 3 * nx, 2 * nx)

    zero = jnp.zeros((8, nz), F32)

    def operate(k, u, v, start, sums):
        line = lax.broadcasted_iota(jnp.int32, (ny, nz), 0)

        def body(turn, carry):
            i = chunk(turn)

            def group(g, carry):
                first, last = [], []
                for j in range(8):
                    x = i * step + g * 8 + j
                    here = u[cells(x), :]
                    after = jnp.broadcast_to(uy[pl.ds(x, 1), :], here.shape)
                    before = jnp.broadcast_to(uy[pl.ds(nx + x, 1), :], here.shape)
                    beside = jnp.where(line == ny - 1, after, pltpu.roll(here, ny - 1, 0))
                    beside = beside + jnp.where(line == 0, before, pltpu.roll(here, 1, 0))
                    beside = beside + u[cells(x + 1), :] + u[cells(x - 1), :]
                    beside = beside + pltpu.roll(here, 1, 1) + pltpu.roll(here, nz - 1, 1)
                    value = (6.0 + mass_shift) * here - beside
                    v[x] = value
                    put_split(x, value)
                    first.append(value[:1])
                    last.append(value[ny - 1 :])
                    carry = sums(x, here, value, carry)
                if k < 2:
                    put_ends(k, i * step + g * 8, first, last)
                return carry

            carry = lax.fori_loop(0, step // 8, group, carry)
            coefs(k, i)
            send_chunk(k, turn, i)
            return carry

        return lax.fori_loop(0, chunks, body, start)

    def first_coefs(i, _):
        coefs(0, i)
        return 0

    lax.fori_loop(0, chunks, first_coefs, 0)

    for load in loads[6:]:
        load.wait()
    tall = nx + 16
    lane = lax.broadcasted_iota(jnp.int32, (tall, 128), 1)
    offset = lax.rem(gy, per_tile) * ny - 32
    window = []
    for e in (0, 1):
        below, own, above = (pltpu.roll(tiles[e, side].astype(F32), lax.rem(128 - offset, 128), 1) for side in range(3))
        window.append(jnp.where(lane + offset < 0, below, jnp.where(lane + offset >= 128, above, own)))
    ranks_x, ranks_y = window
    ranks_behind = pltpu.roll(ranks_x, 1, 0)
    wide = jnp.where(
        lane < 32,
        pltpu.roll(ranks_x, 96, 1),
        jnp.where(lane < 64, ranks_behind, jnp.where(lane < 96, pltpu.roll(ranks_y, 32, 1), pltpu.roll(ranks_y, 65, 1))),
    )
    limits[...] = wide
    level = lambda count: lax.rem(lax.broadcasted_iota(jnp.int32, (count, 128), 1), 32).astype(F32)
    for side, y in enumerate((32 + ny, 31)):
        column = lambda table, t: jnp.broadcast_to(table[:, t : t + 1], (tall, 128))
        own_y, back_y = column(ranks_y, y), column(ranks_y, y - 1)
        limit = jnp.where(
            lane < 32,
            column(ranks_x, y),
            jnp.where(lane < 64, column(ranks_behind, y), jnp.where(lane < 96, own_y, back_y)),
        )
        at = lines + 2 * ny + side * nx
        mask[at : at + nx, :] = jnp.where(level(nx) < limit[8 : 8 + nx], 1.0, 0.0)
    own = lax.rem(lax.broadcasted_iota(jnp.int32, (ny, 128), 1), 32) == lax.broadcasted_iota(jnp.int32, (ny, 128), 0)
    spread = (
        lax.broadcasted_iota(jnp.int32, (128, 128), 0) // 32 == lax.broadcasted_iota(jnp.int32, (128, 128), 1) // 32
    ).astype(F32).astype(BF16)

    def place(x, at):
        line_ranks = jnp.broadcast_to(limits[pl.ds(x + 8, 1), :], (ny, 128))
        picks[pl.ds(pl.multiple_of(at * ny, ny), ny), :] = jnp.where(own, line_ranks, 0.0).astype(BF16)

    def place_own(x, _):
        place(x, x)
        return 0

    lax.fori_loop(0, nx, place_own, 0, unroll=4)
    place(-1, nx)
    place(nx, nx + 1)

    def fill_mask(i, _):
        mask[flat(i), :] = jnp.where(level(rows) < dot(picks[flat(i), :], spread), 1.0, 0.0)
        return 0

    lax.fori_loop(0, chunks, fill_mask, 0)
    mask[lines : lines + 2 * ny, :] = jnp.where(level(2 * ny) < dot(picks[lines : lines + 2 * ny, :], spread), 1.0, 0.0)
    edge_mask[0:ny, :] = jnp.where(segments(ny) == 1, mask[0:ny, :], 0.0)
    edge_mask[ny : 2 * ny, :] = jnp.where(segments(ny) == 0, mask[lines - ny : lines, :], 0.0)
    edge_mask[2 * ny : 2 * ny + nx, :] = jnp.where(segments(nx) == 2, mask[pl.ds(ny - 1, nx, stride=ny), :], 0.0)
    edge_mask[2 * ny + nx : edge, :] = jnp.where(segments(nx) == 3, mask[pl.ds(0, nx, stride=ny), :], 0.0)

    diagonal(u0, inner)
    couple(0, u0, inner)
    pl.semaphore_wait(barrier, ndx + ndy + 2)

    def first_send(turn, _):
        send_chunk(0, turn, chunk(turn))
        return 0

    lax.fori_loop(0, chunks, first_send, 0)
    finish_field(0, u0)

    bu0, u0v0 = operate(
        1, u0, v0, (zero, zero),
        lambda x, here, value, carry: (carry[0] + fold(here * b[x]), carry[1] + fold(here * value)),
    )

    diagonal(u1, inner)
    couple(1, u1, inner)
    finish_field(1, u1)

    bu1, v0u1, u1v1 = operate(
        2, u1, v1, (zero, zero, zero),
        lambda x, here, value, carry: (
            carry[0] + fold(here * b[x]), carry[1] + fold(here * v0[x]), carry[2] + fold(here * value),
        ),
    )

    def row_of(value):
        value = value[:, :128] + value[:, 128:]
        return jnp.sum(value, axis=0, keepdims=True)

    partial = jnp.concatenate(
        [row_of(s) for s in (bu0, u0v0, bu1, v0u1, u1v1)] + [jnp.zeros((3, 128), F32)], axis=0
    )
    part[0] = partial
    got_y[gy] = partial
    along_y = [
        pltpu.make_async_remote_copy(
            src_ref=part.at[0], dst_ref=got_y.at[gy], send_sem=rsend_sem.at[0, k], recv_sem=rrecv_sem.at[0, k],
            device_id=(gx, lax.rem(gy + k, ndy)), device_id_type=MESH,
        )
        for k in range(1, ndy)
    ]
    for copy in along_y:
        copy.start()

    diagonal(u2, flat)
    couple(2, u2, flat)
    for copy in along_y:
        copy.wait()
    partial = jnp.sum(got_y[...], axis=0)
    part[1] = partial
    got_x[gx] = partial
    along_x = [
        pltpu.make_async_remote_copy(
            src_ref=part.at[1], dst_ref=got_x.at[gx], send_sem=rsend_sem.at[1, k], recv_sem=rrecv_sem.at[1, k],
            device_id=(lax.rem(gx + k, ndx), gy), device_id_type=MESH,
        )
        for k in range(1, ndx)
    ]
    for copy in along_x:
        copy.start()
    for copy in all_copies(2):
        copy.wait_recv()
    fix_own(2)
    value = fsplit[0:edge, :]
    more = dot(jnp.concatenate([value, value[:, :128]], axis=1), wd[...])
    uy[2 * nx : 4 * nx, :] = more[2 * ny :]
    u2[0:ny, :] = u2[0:ny, :] + more[:ny]
    u2[lines - ny : lines, :] = u2[lines - ny : lines, :] + more[ny : 2 * ny]
    add_ends(u2, 0, 3 * nx, 2 * nx)
    for k in range(3):
        for copy in all_copies(k):
            copy.wait_send()
    for copy in along_x:
        copy.wait()
    total = jnp.sum(jnp.sum(got_x[...], axis=0), axis=1, keepdims=True)
    s = [total[k : k + 1, :] for k in range(5)]

    alpha0 = s[S_BU0] / s[S_U0V0]
    rz1 = s[S_BU0] - alpha0 * (s[S_U0V0] + s[S_BU1]) + alpha0 * (alpha0 * s[S_V0U1])
    grow = 1.0 + rz1 / s[S_BU0]
    curve = grow * (grow * s[S_U0V0] - 2.0 * (alpha0 * s[S_V0U1])) + alpha0 * (alpha0 * s[S_U1V1])
    alpha1 = rz1 / curve
    on0 = alpha0 + alpha1 * grow
    on1 = -(alpha1 * alpha0)
    scale[0] = jnp.broadcast_to(on0, (8, 128))
    scale[1] = jnp.broadcast_to(on1, (8, 128))


def combine(b, u0, u1, u2, v0, v1, scale, x_any, gap_any, z_any, x_out, gap_out, z_out, sem):
    nx, ny, nz = x_out.shape
    step = 8
    on0, on1 = (jnp.concatenate([jnp.concatenate([scale[k]] * 2, axis=1)] * (ny // 8), axis=0) for k in (0, 1))

    def copies(i):
        here = pl.ds(pl.multiple_of(i * step, step), step)
        return [
            pltpu.make_async_copy(out.at[here], out_any.at[here], sem.at[n, i])
            for n, (out, out_any) in enumerate(((x_out, x_any), (z_out, z_any), (gap_out, gap_any)))
        ]

    def body(i, _):
        for j in range(step):
            x = i * step + j
            at = pl.ds(pl.multiple_of((x + 1) * ny, ny), ny)
            f0, f1 = u0[at, :], u1[at, :]
            x_out[x] = on0 * f0 + on1 * f1
            z_out[x] = f0 - on0 * f1 - on1 * u2[pl.ds(pl.multiple_of(x * ny, ny), ny), :]
            gap_out[x] = b[x] - on0 * v0[x] - on1 * v1[x]
        for copy in copies(i):
            copy.start()
        return 0

    lax.fori_loop(0, nx // step, body, 0)

    def finish(i, _):
        for copy in copies(i):
            copy.wait()
        return 0

    lax.fori_loop(0, nx // step, finish, 0)


def per_device(devs, right_side, block_inverse, basis_left, basis_right, ranks):
    nx, ny, nz = right_side.shape
    ndx, ndy = devs
    lines = nx * ny
    padded = lines + 2 * ny
    edge = 2 * (nx + ny)
    block = jax.ShapeDtypeStruct(right_side.shape, F32)
    framed = jax.ShapeDtypeStruct((padded, nz), F32)
    arrays = (right_side, block_inverse, basis_left, basis_right, ranks)
    fields = pl.pallas_call(
        functools.partial(kernel, devs),
        out_shape=(
            block, framed, framed, jax.ShapeDtypeStruct((lines, nz), F32), block, block,
            jax.ShapeDtypeStruct((2, 8, 128), F32),
        ),
        in_specs=[pl.BlockSpec(memory_space=pltpu.HBM)] * 5,
        out_specs=[pl.BlockSpec(memory_space=pltpu.VMEM)] * 7,
        scratch_shapes=[
            pltpu.VMEM((nz, nz), F32),
            pltpu.VMEM((4, 32, nz), F32),
            pltpu.VMEM((2, 3, nx + 16, 128), jnp.int32),
            pltpu.VMEM((nx + 16, 128), F32),
            pltpu.VMEM((lines + 2 * ny, 128), BF16),
            pltpu.VMEM((3 * nz, nz), BF16),
            pltpu.VMEM((2 * nz, 256), BF16),
            pltpu.VMEM((384, nz), BF16),
            pltpu.VMEM((lines + edge, 128), F32),
            pltpu.VMEM((edge, 128), F32),
            pltpu.VMEM((lines, 2 * nz), BF16),
            pltpu.VMEM((16 * ny, 256), BF16),
            pltpu.VMEM((2 * edge, 256), BF16),
            pltpu.VMEM((3, padded, 128), F32),
            pltpu.VMEM((3, edge, 128), F32),
            pltpu.VMEM((3, edge, 128), F32),
            pltpu.VMEM((2, 2, nx, nz), F32),
            pltpu.VMEM((2, edge, nz), F32),
            pltpu.VMEM((2, 4, 8, 128), F32),
            pltpu.VMEM((2, 4, 8, 128), F32),
            pltpu.VMEM((4 * nx, nz), F32),
            pltpu.VMEM((2, 8, 128), F32),
            pltpu.VMEM((ndy, 8, 128), F32),
            pltpu.VMEM((ndx, 8, 128), F32),
            pltpu.SemaphoreType.DMA((24,)),
            pltpu.SemaphoreType.DMA((3, 2, 2)),
            pltpu.SemaphoreType.DMA((3, 2, 2)),
            pltpu.SemaphoreType.DMA((3, 2, 2, nx // 16)),
            pltpu.SemaphoreType.DMA((3, 2, 2, nx // 16)),
            pltpu.SemaphoreType.DMA((2, 4)),
            pltpu.SemaphoreType.DMA((2, 4)),
            pltpu.SemaphoreType.DMA((2, ndy)),
            pltpu.SemaphoreType.DMA((2, ndy)),
        ],
        compiler_params=pltpu.CompilerParams(
            collective_id=0, has_side_effects=True, vmem_limit_bytes=32 * 1024 * 1024
        ),
    )(*(pltpu.with_memory_space_constraint(array, pltpu.HBM) for array in arrays))
    return pl.pallas_call(
        combine,
        out_shape=(block, block, block),
        in_specs=[pl.BlockSpec(memory_space=pltpu.VMEM)] * 7,
        out_specs=[pl.BlockSpec(memory_space=pltpu.HBM)] * 3,
        scratch_shapes=[pltpu.VMEM((nx, ny, nz), F32)] * 3 + [pltpu.SemaphoreType.DMA((3, nx // 8))],
        compiler_params=pltpu.CompilerParams(vmem_limit_bytes=32 * 1024 * 1024),
    )(*fields)


def solution(mesh):
    devs = (mesh.shape["gx"], mesh.shape["gy"])
    return jax.shard_map(
        functools.partial(per_device, devs),
        mesh=mesh,
        in_specs=(P("gx", "gy", None), P(), P(), P(), P()),
        out_specs=(P("gx", "gy", None),) * 3,
        check_vma=False,
    )
```

```python
import functools

import jax
import jax.numpy as jnp
from jax import lax
from jax.experimental import pallas as pl
from jax.experimental.pallas import tpu as pltpu
from jax.sharding import PartitionSpec as P

F32 = jnp.float32
BF16 = jnp.bfloat16
MESH = pl.DeviceIdType.MESH

mass_shift = 0.05

S_BU0, S_U0V0, S_BU1, S_V0U1, S_U1V1 = range(5)


def halves(value):
    high = value.astype(BF16)
    return high, (value - high.astype(F32)).astype(BF16)


def dot(a, b):
    return lax.dot_general(a, b, (((1,), (0,)), ((), ())), preferred_element_type=F32)


def fold(value):
    rows, width = value.shape
    return jnp.sum(value.reshape(rows // 8, 8, width), axis=0)


def kernel(
    devs, b_any, binv_any, left_any, right_any, ranks_any,
    b, u0, u1, u2, v0, v1, scale,
    binv, bases, tiles, limits, picks, wb, wc, wd, mask, edge_mask, split, dsplit, fsplit,
    c, coef_send, coef_recv, raw_send, raw_recv, corner_send, corner_recv, uy, part, got_y, got_x,
    load_sem, xsend_sem, xrecv_sem, ysend_sem, yrecv_sem, ksend_sem, krecv_sem, rsend_sem, rrecv_sem,
):
    ndx, ndy = devs
    nx, ny, nz = b.shape
    lines = nx * ny
    edge = 2 * ny + 2 * nx
    step = 16
    rows = step * ny
    chunks = nx // step
    gx = lax.axis_index("gx")
    gy = lax.axis_index("gy")
    east, west = lax.rem(gx + 1, ndx), lax.rem(gx + ndx - 1, ndx)
    north, south = lax.rem(gy + 1, ndy), lax.rem(gy + ndy - 1, ndy)
    diagonals = ((east, north), (east, south), (west, north), (west, south))

    barrier = pltpu.get_barrier_semaphore()
    for k in range(1, ndy):
        pl.semaphore_signal(barrier, 1, device_id=(gx, lax.rem(gy + k, ndy)), device_id_type=MESH)
    for k in range(1, ndx):
        pl.semaphore_signal(barrier, 1, device_id=(lax.rem(gx + k, ndx), gy), device_id_type=MESH)
    for to in diagonals:
        pl.semaphore_signal(barrier, 1, device_id=to, device_id_type=MESH)

    per_tile = 128 // ny
    tile_count = ndy // per_tile
    tile = gy // per_tile
    row_starts = (
        (0, lax.rem(gx * nx + ndx * nx - 8, ndx * nx), 8),
        (8, gx * nx, nx),
        (8 + nx, lax.rem(gx * nx + nx, ndx * nx), 8),
    )
    loads = [
        pltpu.make_async_copy(binv_any.at[0], binv, load_sem.at[0]),
        pltpu.make_async_copy(right_any.at[0, 0], bases.at[0], load_sem.at[1]),
        pltpu.make_async_copy(left_any.at[0, 0], bases.at[1], load_sem.at[2]),
        pltpu.make_async_copy(right_any.at[1, 0], bases.at[2], load_sem.at[3]),
        pltpu.make_async_copy(left_any.at[1, 0], bases.at[3], load_sem.at[4]),
        pltpu.make_async_copy(b_any, b, load_sem.at[5]),
    ]
    for e in (0, 1):
        for side in (0, 1, 2):
            col = pl.multiple_of(lax.rem(tile + side + tile_count - 1, tile_count) * 128, 128)
            for to, start, count in row_starts:
                loads.append(
                    pltpu.make_async_copy(
                        ranks_any.at[e, 0, pl.ds(pl.multiple_of(start, 8), count), pl.ds(col, 128)],
                        tiles.at[e, side, pl.ds(to, count)],
                        load_sem.at[len(loads)],
                    )
                )
    for load in loads:
        load.start()

    def cells(x):
        return pl.ds(pl.multiple_of((x + 1) * ny, ny), ny)

    def flat(i):
        return pl.ds(pl.multiple_of(i * rows, rows), rows)

    def inner(i):
        return pl.ds(pl.multiple_of(i * rows + ny, ny), rows)

    def segments(count):
        return lax.broadcasted_iota(jnp.int32, (count, 128), 1) // 32

    for load in loads[1:5]:
        load.wait()
    factors = bases[...].reshape(4 * 32, nz)
    high, low = halves(factors.T)
    wc[0:nz, 0:128] = high
    wc[0:nz, 128:256] = low
    wc[nz : 2 * nz, 0:128] = high
    wc[nz : 2 * nz, 128:256] = jnp.zeros((nz, 128), BF16)

    loads[5].wait()

    def put_split(x, value):
        at = pl.ds(pl.multiple_of(x * ny, ny), ny)
        high, low = halves(value)
        split[at, 0:nz] = high
        split[at, nz : 2 * nz] = low

    def put_ends(k, start, first, last):
        here = pl.ds(pl.multiple_of(start, 8), 8)
        raw_send[k, 0, here, :] = jnp.concatenate(first, axis=0)
        raw_send[k, 1, here, :] = jnp.concatenate(last, axis=0)

    def first_split(g, _):
        first, last = [], []
        for j in range(8):
            value = b[g * 8 + j]
            put_split(g * 8 + j, value)
            first.append(value[:1])
            last.append(value[ny - 1 :])
        put_ends(0, g * 8, first, last)
        return 0

    lax.fori_loop(0, nx // 8, first_split, 0)

    def coefs(k, i):
        both = dot(split[flat(i), :], wc[...])
        c[k, inner(i), :] = both[:, :128] + both[:, 128:]

    def pack_y(k, i):
        seg = segments(step)
        base = pl.multiple_of(i * rows + ny, ny)
        first, second = (c[k, pl.ds(base + n, step, stride=ny), :] for n in (0, 1))
        last, before = (c[k, pl.ds(base + ny - n, step, stride=ny), :] for n in (1, 2))
        coef_send[k, pl.ds(pl.multiple_of(2 * ny + i * step, step), step), :] = jnp.where(
            seg == 3, pltpu.roll(second, 32, 1), first
        )
        coef_send[k, pl.ds(pl.multiple_of(2 * ny + nx + i * step, step), step), :] = jnp.where(
            seg == 2, pltpu.roll(before, 96, 1), last
        )

    def pack_x(k, side):
        seg = segments(ny)
        x, behind, where, turn = ((0, 1, 1, 32), (nx - 1, nx - 2, 0, 96))[side]
        own = c[k, cells(x), :]
        coef_send[k, pl.ds(side * ny, ny), :] = jnp.where(seg == where, pltpu.roll(c[k, cells(behind), :], turn, 1), own)
        if k < 2:
            corner_send[k, 2 * (1 - side)] = jnp.broadcast_to(own[ny - 1 :], (8, 128))
            corner_send[k, 2 * (1 - side) + 1] = jnp.broadcast_to(own[:1], (8, 128))

    fields = (b, v0)

    def x_copies(k, side):
        to = ((west, gy), (east, gy))[side]
        mine, theirs = side * ny, (1 - side) * ny
        pairs = [(coef_send.at[k, pl.ds(mine, ny)], coef_recv.at[k, pl.ds(theirs, ny)])]
        if k < 2:
            pairs.append((fields[k].at[(0, nx - 1)[side]], raw_recv.at[k, pl.ds(theirs, ny)]))
        copies = [
            pltpu.make_async_remote_copy(
                src_ref=src, dst_ref=dst, send_sem=xsend_sem.at[k, side, n], recv_sem=xrecv_sem.at[k, side, n],
                device_id=to, device_id_type=MESH,
            )
            for n, (src, dst) in enumerate(pairs)
        ]
        if k < 2:
            for n in (2 * (1 - side), 2 * (1 - side) + 1):
                copies.append(
                    pltpu.make_async_remote_copy(
                        src_ref=corner_send.at[k, n], dst_ref=corner_recv.at[k, n],
                        send_sem=ksend_sem.at[k, n], recv_sem=krecv_sem.at[k, n],
                        device_id=diagonals[n], device_id_type=MESH,
                    )
                )
        return copies

    def y_copies(k, side, i):
        count = nx if k == 0 else step
        here = pl.ds(pl.multiple_of(i * count, step), count)
        there = pl.ds(pl.multiple_of(2 * ny + side * nx + i * count, step), count)
        pairs = [(coef_send.at[k, there], coef_recv.at[k, there])]
        if k < 2:
            pairs.append((raw_send.at[k, side, here], raw_recv.at[k, there]))
        return [
            pltpu.make_async_remote_copy(
                src_ref=src, dst_ref=dst, send_sem=ysend_sem.at[k, side, n, i], recv_sem=yrecv_sem.at[k, side, n, i],
                device_id=(gx, (south, north)[side]), device_id_type=MESH,
            )
            for n, (src, dst) in enumerate(pairs)
        ]

    def send_chunk(k, turn, i):
        for side in (0, 1):

            @pl.when(turn == side)
            def _():
                pack_x(k, side)
                for copy in x_copies(k, side):
                    copy.start()

        pack_y(k, i)
        for side in (0, 1):
            for copy in y_copies(k, side, i):
                copy.start()

    def all_copies(k):
        return [copy for side in (0, 1) for copy in x_copies(k, side)] + [
            copy for side in (0, 1) for i in range(1 if k == 0 else chunks) for copy in y_copies(k, side, i)
        ]

    def chunk(turn):
        return jnp.where(turn == 0, 0, jnp.where(turn == 1, chunks - 1, turn - 1))

    def diagonal(out, place):
        def body(i, _):
            value = split[flat(i), :]
            out[place(i), :] = dot(jnp.concatenate([value, value[:, :nz]], axis=1), wb[...])
            return 0

        lax.fori_loop(0, chunks, body, 0)

    def couple(k, out, place):
        seg = segments(ny)
        line = lax.broadcasted_iota(jnp.int32, (ny, 128), 0)
        use_after = (seg == 2) & (line < ny - 1)
        use_before = (seg == 3) & (line > 0)

        def body(i, _):
            for j in range(step):
                x = i * step + j
                here = c[k, cells(x), :]
                coef = jnp.where(seg == 0, c[k, cells(x + 1), :], jnp.where(seg == 1, c[k, cells(x - 1), :], 0.0))
                coef = jnp.where(use_after, pltpu.roll(here, ny - 1, 0), coef)
                coef = jnp.where(use_before, pltpu.roll(here, 1, 0), coef)
                coef = coef * mask[pl.ds(pl.multiple_of(x * ny, ny), ny), :]
                high, low = halves(coef)
                dsplit[j * ny : (j + 1) * ny, 0:128] = high
                dsplit[j * ny : (j + 1) * ny, 128:256] = low
            value = dsplit[...]
            out[place(i), :] = out[place(i), :] + dot(jnp.concatenate([value, value[:, :128]], axis=1), wd[...])
            return 0

        lax.fori_loop(0, chunks, body, 0)

    def add_ends(out, at, first, last):
        line = lax.broadcasted_iota(jnp.int32, (8, nz), 0)

        def body(x, _):
            head = pl.ds(pl.multiple_of(at + x * ny, 8), 8)
            tail = pl.ds(pl.multiple_of(at + x * ny + ny - 8, 8), 8)
            more = jnp.broadcast_to(fsplit_out[pl.ds(first + x, 1), :], (8, nz))
            out[head, :] = out[head, :] + jnp.where(line == 0, more, 0.0)
            more = jnp.broadcast_to(fsplit_out[pl.ds(last + x, 1), :], (8, nz))
            out[tail, :] = out[tail, :] + jnp.where(line == 7, more, 0.0)
            return 0

        lax.fori_loop(0, nx, body, 0, unroll=8)

    fsplit_out = uy

    def put_fix(at, value):
        high, low = halves(value)
        fsplit[at : at + value.shape[0], 0:128] = high
        fsplit[at : at + value.shape[0], 128:256] = low

    def fix_own(k):
        put_fix(0, coef_recv[k] * edge_mask[...])

    def fix_halo(k):
        got = lambda at, count: coef_recv[k, at : at + count, :]
        corner = lambda n, count: jnp.broadcast_to(corner_recv[k, n][:1], (count, 128))
        ws, wn, es, en = range(4)
        seg = segments(ny)
        line = lax.broadcasted_iota(jnp.int32, (ny, 128), 0)
        for side, (lo, hi) in enumerate(((ws, wn), (es, en))):
            here = got(side * ny, ny)
            after = jnp.where(line == ny - 1, corner(hi, ny), pltpu.roll(here, ny - 1, 0))
            before = jnp.where(line == 0, corner(lo, ny), pltpu.roll(here, 1, 0))
            if side == 0:
                ahead, behind = c[k, cells(0), :], pltpu.roll(here, 32, 1)
            else:
                ahead, behind = pltpu.roll(here, 96, 1), c[k, cells(nx - 1), :]
            coef = jnp.where(seg == 0, ahead, jnp.where(seg == 1, behind, jnp.where(seg == 2, after, before)))
            put_fix(edge + side * ny, coef * mask[lines + side * ny : lines + (side + 1) * ny, :])
        seg = segments(nx)
        line = lax.broadcasted_iota(jnp.int32, (nx, 128), 0)
        for side, (lo, hi) in enumerate(((wn, en), (ws, es))):
            at = 2 * ny + side * nx
            here = got(at, nx)
            ahead = jnp.where(line == nx - 1, corner(hi, nx), pltpu.roll(here, nx - 1, 0))
            behind = jnp.where(line == 0, corner(lo, nx), pltpu.roll(here, 1, 0))
            if side == 0:
                after = pltpu.roll(here, 96, 1)
                before = c[k, pl.ds(ny + ny - 1, nx, stride=ny), :]
            else:
                after = c[k, pl.ds(ny, nx, stride=ny), :]
                before = pltpu.roll(here, 32, 1)
            coef = jnp.where(seg == 0, ahead, jnp.where(seg == 1, behind, jnp.where(seg == 2, after, before)))
            put_fix(edge + at, coef * mask[lines + at : lines + at + nx, :])

    def finish_field(k, u):
        for copy in all_copies(k):
            copy.wait_recv()
        fix_own(k)
        fix_halo(k)
        high, low = halves(raw_recv[k])
        value = fsplit[...]
        more = dot(jnp.concatenate([value, value[:, :128]], axis=1), wd[...])
        halo = more[edge:] + dot(jnp.concatenate([high, low, high], axis=1), wb[...])
        u[0:ny, :] = halo[:ny]
        u[(nx + 1) * ny : (nx + 2) * ny, :] = halo[ny : 2 * ny]
        uy[0 : 2 * nx, :] = halo[2 * ny :]
        uy[2 * nx : 4 * nx, :] = more[2 * ny : edge]
        u[cells(0), :] = u[cells(0), :] + more[:ny]
        u[cells(nx - 1), :] = u[cells(nx - 1), :] + more[ny : 2 * ny]
        add_ends(u, ny, 3 * nx, 2 * nx)

    zero = jnp.zeros((8, nz), F32)

    def operate(k, u, v, start, sums):
        line = lax.broadcasted_iota(jnp.int32, (ny, nz), 0)

        def body(turn, carry):
            i = chunk(turn)

            def group(g, carry):
                first, last = [], []
                for j in range(8):
                    x = i * step + g * 8 + j
                    here = u[cells(x), :]
                    after = jnp.broadcast_to(uy[pl.ds(x, 1), :], here.shape)
                    before = jnp.broadcast_to(uy[pl.ds(nx + x, 1), :], here.shape)
                    beside = jnp.where(line == ny - 1, after, pltpu.roll(here, ny - 1, 0))
                    beside = beside + jnp.where(line == 0, before, pltpu.roll(here, 1, 0))
                    beside = beside + u[cells(x + 1), :] + u[cells(x - 1), :]
                    beside = beside + pltpu.roll(here, 1, 1) + pltpu.roll(here, nz - 1, 1)
                    value = (6.0 + mass_shift) * here - beside
                    v[x] = value
                    put_split(x, value)
                    first.append(value[:1])
                    last.append(value[ny - 1 :])
                    carry = sums(x, here, value, carry)
                if k < 2:
                    put_ends(k, i * step + g * 8, first, last)
                return carry

            carry = lax.fori_loop(0, step // 8, group, carry)
            coefs(k, i)
            send_chunk(k, turn, i)
            return carry

        return lax.fori_loop(0, chunks, body, start)

    def first_coefs(i, _):
        coefs(0, i)
        pack_y(0, i)
        return 0

    lax.fori_loop(0, chunks, first_coefs, 0)
    for side in (0, 1):
        pack_x(0, side)

    pl.semaphore_wait(barrier, ndx + ndy + 2)
    for copy in all_copies(0):
        copy.start()

    loads[0].wait()
    high, low = halves(binv[...].T)
    wb[0:nz, :] = high
    wb[nz : 2 * nz, :] = high
    wb[2 * nz : 3 * nz, :] = low
    swapped = jnp.concatenate([bases[1], bases[0], bases[3], bases[2]], axis=0)
    high, low = halves(swapped)
    wd[0:128, :] = high
    wd[128:256, :] = high
    wd[256:384, :] = low

    for k in range(3):
        c[k, 0:ny, :] = jnp.zeros((ny, 128), F32)
        c[k, (nx + 1) * ny : (nx + 2) * ny, :] = jnp.zeros((ny, 128), F32)

    for load in loads[6:]:
        load.wait()
    tall = nx + 16
    lane = lax.broadcasted_iota(jnp.int32, (tall, 128), 1)
    offset = lax.rem(gy, per_tile) * ny - 32
    window = []
    for e in (0, 1):
        below, own, above = (pltpu.roll(tiles[e, side].astype(F32), lax.rem(128 - offset, 128), 1) for side in range(3))
        window.append(jnp.where(lane + offset < 0, below, jnp.where(lane + offset >= 128, above, own)))
    ranks_x, ranks_y = window
    ranks_behind = pltpu.roll(ranks_x, 1, 0)
    wide = jnp.where(
        lane < 32,
        pltpu.roll(ranks_x, 96, 1),
        jnp.where(lane < 64, ranks_behind, jnp.where(lane < 96, pltpu.roll(ranks_y, 32, 1), pltpu.roll(ranks_y, 65, 1))),
    )
    limits[...] = wide
    level = lambda count: lax.rem(lax.broadcasted_iota(jnp.int32, (count, 128), 1), 32).astype(F32)
    for side, y in enumerate((32 + ny, 31)):
        column = lambda table, t: jnp.broadcast_to(table[:, t : t + 1], (tall, 128))
        own_y, back_y = column(ranks_y, y), column(ranks_y, y - 1)
        limit = jnp.where(
            lane < 32,
            column(ranks_x, y),
            jnp.where(lane < 64, column(ranks_behind, y), jnp.where(lane < 96, own_y, back_y)),
        )
        at = lines + 2 * ny + side * nx
        mask[at : at + nx, :] = jnp.where(level(nx) < limit[8 : 8 + nx], 1.0, 0.0)
    own = lax.rem(lax.broadcasted_iota(jnp.int32, (ny, 128), 1), 32) == lax.broadcasted_iota(jnp.int32, (ny, 128), 0)
    spread = (
        lax.broadcasted_iota(jnp.int32, (128, 128), 0) // 32 == lax.broadcasted_iota(jnp.int32, (128, 128), 1) // 32
    ).astype(F32).astype(BF16)

    def place(x, at):
        line_ranks = jnp.broadcast_to(limits[pl.ds(x + 8, 1), :], (ny, 128))
        picks[pl.ds(pl.multiple_of(at * ny, ny), ny), :] = jnp.where(own, line_ranks, 0.0).astype(BF16)

    def place_own(x, _):
        place(x, x)
        return 0

    lax.fori_loop(0, nx, place_own, 0, unroll=4)
    place(-1, nx)
    place(nx, nx + 1)

    def fill_mask(i, _):
        mask[flat(i), :] = jnp.where(level(rows) < dot(picks[flat(i), :], spread), 1.0, 0.0)
        return 0

    lax.fori_loop(0, chunks, fill_mask, 0)
    mask[lines : lines + 2 * ny, :] = jnp.where(level(2 * ny) < dot(picks[lines : lines + 2 * ny, :], spread), 1.0, 0.0)
    edge_mask[0:ny, :] = jnp.where(segments(ny) == 1, mask[0:ny, :], 0.0)
    edge_mask[ny : 2 * ny, :] = jnp.where(segments(ny) == 0, mask[lines - ny : lines, :], 0.0)
    edge_mask[2 * ny : 2 * ny + nx, :] = jnp.where(segments(nx) == 2, mask[pl.ds(ny - 1, nx, stride=ny), :], 0.0)
    edge_mask[2 * ny + nx : edge, :] = jnp.where(segments(nx) == 3, mask[pl.ds(0, nx, stride=ny), :], 0.0)

    diagonal(u0, inner)
    couple(0, u0, inner)
    finish_field(0, u0)

    bu0, u0v0 = operate(
        1, u0, v0, (zero, zero),
        lambda x, here, value, carry: (carry[0] + fold(here * b[x]), carry[1] + fold(here * value)),
    )

    diagonal(u1, inner)
    couple(1, u1, inner)
    finish_field(1, u1)

    bu1, v0u1, u1v1 = operate(
        2, u1, v1, (zero, zero, zero),
        lambda x, here, value, carry: (
            carry[0] + fold(here * b[x]), carry[1] + fold(here * v0[x]), carry[2] + fold(here * value),
        ),
    )

    def row_of(value):
        value = value[:, :128] + value[:, 128:]
        return jnp.sum(value, axis=0, keepdims=True)

    partial = jnp.concatenate(
        [row_of(s) for s in (bu0, u0v0, bu1, v0u1, u1v1)] + [jnp.zeros((3, 128), F32)], axis=0
    )
    part[0] = partial
    got_y[gy] = partial
    along_y = [
        pltpu.make_async_remote_copy(
            src_ref=part.at[0], dst_ref=got_y.at[gy], send_sem=rsend_sem.at[0, k], recv_sem=rrecv_sem.at[0, k],
            device_id=(gx, lax.rem(gy + k, ndy)), device_id_type=MESH,
        )
        for k in range(1, ndy)
    ]
    for copy in along_y:
        copy.start()

    diagonal(u2, flat)
    couple(2, u2, flat)
    for copy in along_y:
        copy.wait()
    partial = jnp.sum(got_y[...], axis=0)
    part[1] = partial
    got_x[gx] = partial
    along_x = [
        pltpu.make_async_remote_copy(
            src_ref=part.at[1], dst_ref=got_x.at[gx], send_sem=rsend_sem.at[1, k], recv_sem=rrecv_sem.at[1, k],
            device_id=(lax.rem(gx + k, ndx), gy), device_id_type=MESH,
        )
        for k in range(1, ndx)
    ]
    for copy in along_x:
        copy.start()
    for copy in all_copies(2):
        copy.wait_recv()
    fix_own(2)
    value = fsplit[0:edge, :]
    more = dot(jnp.concatenate([value, value[:, :128]], axis=1), wd[...])
    uy[2 * nx : 4 * nx, :] = more[2 * ny :]
    u2[0:ny, :] = u2[0:ny, :] + more[:ny]
    u2[lines - ny : lines, :] = u2[lines - ny : lines, :] + more[ny : 2 * ny]
    add_ends(u2, 0, 3 * nx, 2 * nx)
    for k in range(3):
        for copy in all_copies(k):
            copy.wait_send()
    for copy in along_x:
        copy.wait()
    total = jnp.sum(jnp.sum(got_x[...], axis=0), axis=1, keepdims=True)
    s = [total[k : k + 1, :] for k in range(5)]

    alpha0 = s[S_BU0] / s[S_U0V0]
    rz1 = s[S_BU0] - alpha0 * (s[S_U0V0] + s[S_BU1]) + alpha0 * (alpha0 * s[S_V0U1])
    grow = 1.0 + rz1 / s[S_BU0]
    curve = grow * (grow * s[S_U0V0] - 2.0 * (alpha0 * s[S_V0U1])) + alpha0 * (alpha0 * s[S_U1V1])
    alpha1 = rz1 / curve
    on0 = alpha0 + alpha1 * grow
    on1 = -(alpha1 * alpha0)
    scale[0] = jnp.broadcast_to(on0, (8, 128))
    scale[1] = jnp.broadcast_to(on1, (8, 128))


def combine(b, u0, u1, u2, v0, v1, scale, x_any, gap_any, z_any, x_out, gap_out, z_out, sem):
    nx, ny, nz = x_out.shape
    step = 8
    on0, on1 = (jnp.concatenate([jnp.concatenate([scale[k]] * 2, axis=1)] * (ny // 8), axis=0) for k in (0, 1))

    def copies(i):
        here = pl.ds(pl.multiple_of(i * step, step), step)
        return [
            pltpu.make_async_copy(out.at[here], out_any.at[here], sem.at[n, i])
            for n, (out, out_any) in enumerate(((x_out, x_any), (z_out, z_any), (gap_out, gap_any)))
        ]

    def body(i, _):
        for j in range(step):
            x = i * step + j
            at = pl.ds(pl.multiple_of((x + 1) * ny, ny), ny)
            f0, f1 = u0[at, :], u1[at, :]
            x_out[x] = on0 * f0 + on1 * f1
            z_out[x] = f0 - on0 * f1 - on1 * u2[pl.ds(pl.multiple_of(x * ny, ny), ny), :]
            gap_out[x] = b[x] - on0 * v0[x] - on1 * v1[x]
        for copy in copies(i):
            copy.start()
        return 0

    lax.fori_loop(0, nx // step, body, 0)

    def finish(i, _):
        for copy in copies(i):
            copy.wait()
        return 0

    lax.fori_loop(0, nx // step, finish, 0)


def per_device(devs, right_side, block_inverse, basis_left, basis_right, ranks):
    nx, ny, nz = right_side.shape
    ndx, ndy = devs
    lines = nx * ny
    padded = lines + 2 * ny
    edge = 2 * (nx + ny)
    block = jax.ShapeDtypeStruct(right_side.shape, F32)
    framed = jax.ShapeDtypeStruct((padded, nz), F32)
    arrays = (right_side, block_inverse, basis_left, basis_right, ranks)
    fields = pl.pallas_call(
        functools.partial(kernel, devs),
        out_shape=(
            block, framed, framed, jax.ShapeDtypeStruct((lines, nz), F32), block, block,
            jax.ShapeDtypeStruct((2, 8, 128), F32),
        ),
        in_specs=[pl.BlockSpec(memory_space=pltpu.HBM)] * 5,
        out_specs=[pl.BlockSpec(memory_space=pltpu.VMEM)] * 7,
        scratch_shapes=[
            pltpu.VMEM((nz, nz), F32),
            pltpu.VMEM((4, 32, nz), F32),
            pltpu.VMEM((2, 3, nx + 16, 128), jnp.int32),
            pltpu.VMEM((nx + 16, 128), F32),
            pltpu.VMEM((lines + 2 * ny, 128), BF16),
            pltpu.VMEM((3 * nz, nz), BF16),
            pltpu.VMEM((2 * nz, 256), BF16),
            pltpu.VMEM((384, nz), BF16),
            pltpu.VMEM((lines + edge, 128), F32),
            pltpu.VMEM((edge, 128), F32),
            pltpu.VMEM((lines, 2 * nz), BF16),
            pltpu.VMEM((16 * ny, 256), BF16),
            pltpu.VMEM((2 * edge, 256), BF16),
            pltpu.VMEM((3, padded, 128), F32),
            pltpu.VMEM((3, edge, 128), F32),
            pltpu.VMEM((3, edge, 128), F32),
            pltpu.VMEM((2, 2, nx, nz), F32),
            pltpu.VMEM((2, edge, nz), F32),
            pltpu.VMEM((2, 4, 8, 128), F32),
            pltpu.VMEM((2, 4, 8, 128), F32),
            pltpu.VMEM((4 * nx, nz), F32),
            pltpu.VMEM((2, 8, 128), F32),
            pltpu.VMEM((ndy, 8, 128), F32),
            pltpu.VMEM((ndx, 8, 128), F32),
            pltpu.SemaphoreType.DMA((24,)),
            pltpu.SemaphoreType.DMA((3, 2, 2)),
            pltpu.SemaphoreType.DMA((3, 2, 2)),
            pltpu.SemaphoreType.DMA((3, 2, 2, nx // 16)),
            pltpu.SemaphoreType.DMA((3, 2, 2, nx // 16)),
            pltpu.SemaphoreType.DMA((2, 4)),
            pltpu.SemaphoreType.DMA((2, 4)),
            pltpu.SemaphoreType.DMA((2, ndy)),
            pltpu.SemaphoreType.DMA((2, ndy)),
        ],
        compiler_params=pltpu.CompilerParams(
            collective_id=0, has_side_effects=True, vmem_limit_bytes=32 * 1024 * 1024
        ),
    )(*(pltpu.with_memory_space_constraint(array, pltpu.HBM) for array in arrays))
    return pl.pallas_call(
        combine,
        out_shape=(block, block, block),
        in_specs=[pl.BlockSpec(memory_space=pltpu.VMEM)] * 7,
        out_specs=[pl.BlockSpec(memory_space=pltpu.HBM)] * 3,
        scratch_shapes=[pltpu.VMEM((nx, ny, nz), F32)] * 3 + [pltpu.SemaphoreType.DMA((3, nx // 8))],
        compiler_params=pltpu.CompilerParams(vmem_limit_bytes=32 * 1024 * 1024),
    )(*fields)


def solution(mesh):
    devs = (mesh.shape["gx"], mesh.shape["gy"])
    return jax.shard_map(
        functools.partial(per_device, devs),
        mesh=mesh,
        in_specs=(P("gx", "gy", None), P(), P(), P(), P()),
        out_specs=(P("gx", "gy", None),) * 3,
        check_vma=False,
    )
```

```python
import functools

import jax
import jax.numpy as jnp
from jax import lax
from jax.experimental import pallas as pl
from jax.experimental.pallas import tpu as pltpu
from jax.sharding import PartitionSpec as P

F32 = jnp.float32
BF16 = jnp.bfloat16
MESH = pl.DeviceIdType.MESH

mass_shift = 0.05

S_BU0, S_U0V0, S_BU1, S_V0U1, S_U1V1 = range(5)


def halves(value):
    high = value.astype(BF16)
    return high, (value - high.astype(F32)).astype(BF16)


def dot(a, b):
    return lax.dot_general(a, b, (((1,), (0,)), ((), ())), preferred_element_type=F32)


def fold(value):
    rows, width = value.shape
    return jnp.sum(value.reshape(rows // 8, 8, width), axis=0)


def kernel(
    devs, b_any, binv_any, left_any, right_any, ranks_any,
    b, u0, u1, u2, v0, v1, scale,
    binv, bases, tiles, limits, picks, wb, wc, wd, mask, edge_mask, split, dsplit, fsplit,
    c, coef_send, coef_recv, raw_send, raw_recv, corner_send, corner_recv, uy, part, got_y, got_x,
    load_sem, xsend_sem, xrecv_sem, ysend_sem, yrecv_sem, ksend_sem, krecv_sem, rsend_sem, rrecv_sem,
):
    ndx, ndy = devs
    nx, ny, nz = b.shape
    lines = nx * ny
    edge = 2 * ny + 2 * nx
    step = 16
    rows = step * ny
    chunks = nx // step
    gx = lax.axis_index("gx")
    gy = lax.axis_index("gy")
    east, west = lax.rem(gx + 1, ndx), lax.rem(gx + ndx - 1, ndx)
    north, south = lax.rem(gy + 1, ndy), lax.rem(gy + ndy - 1, ndy)
    diagonals = ((east, north), (east, south), (west, north), (west, south))

    per_tile = 128 // ny
    tile_count = ndy // per_tile
    tile = gy // per_tile
    row_starts = (
        (0, lax.rem(gx * nx + ndx * nx - 8, ndx * nx), 8),
        (8, gx * nx, nx),
        (8 + nx, lax.rem(gx * nx + nx, ndx * nx), 8),
    )
    loads = [
        pltpu.make_async_copy(binv_any.at[0], binv, load_sem.at[0]),
        pltpu.make_async_copy(right_any.at[0, 0], bases.at[0], load_sem.at[1]),
        pltpu.make_async_copy(left_any.at[0, 0], bases.at[1], load_sem.at[2]),
        pltpu.make_async_copy(right_any.at[1, 0], bases.at[2], load_sem.at[3]),
        pltpu.make_async_copy(left_any.at[1, 0], bases.at[3], load_sem.at[4]),
        pltpu.make_async_copy(b_any, b, load_sem.at[5]),
    ]
    for e in (0, 1):
        for side in (0, 1, 2):
            col = pl.multiple_of(lax.rem(tile + side + tile_count - 1, tile_count) * 128, 128)
            for to, start, count in row_starts:
                loads.append(
                    pltpu.make_async_copy(
                        ranks_any.at[e, 0, pl.ds(pl.multiple_of(start, 8), count), pl.ds(col, 128)],
                        tiles.at[e, side, pl.ds(to, count)],
                        load_sem.at[len(loads)],
                    )
                )
    for load in loads[1:6]:
        load.start()

    barrier = pltpu.get_barrier_semaphore()
    for k in range(1, ndy):
        pl.semaphore_signal(barrier, 1, device_id=(gx, lax.rem(gy + k, ndy)), device_id_type=MESH)
    for k in range(1, ndx):
        pl.semaphore_signal(barrier, 1, device_id=(lax.rem(gx + k, ndx), gy), device_id_type=MESH)
    for to in diagonals:
        pl.semaphore_signal(barrier, 1, device_id=to, device_id_type=MESH)

    for load in loads[:1] + loads[6:]:
        load.start()

    def cells(x):
        return pl.ds(pl.multiple_of((x + 1) * ny, ny), ny)

    def flat(i):
        return pl.ds(pl.multiple_of(i * rows, rows), rows)

    def inner(i):
        return pl.ds(pl.multiple_of(i * rows + ny, ny), rows)

    def segments(count):
        return lax.broadcasted_iota(jnp.int32, (count, 128), 1) // 32

    for load in loads[1:5]:
        load.wait()
    factors = bases[...].reshape(4 * 32, nz)
    high, low = halves(factors.T)
    wc[0:nz, 0:128] = high
    wc[0:nz, 128:256] = low
    wc[nz : 2 * nz, 0:128] = high
    wc[nz : 2 * nz, 128:256] = jnp.zeros((nz, 128), BF16)

    loads[5].wait()

    def put_split(x, value):
        at = pl.ds(pl.multiple_of(x * ny, ny), ny)
        high, low = halves(value)
        split[at, 0:nz] = high
        split[at, nz : 2 * nz] = low

    def put_ends(k, start, first, last):
        here = pl.ds(pl.multiple_of(start, 8), 8)
        raw_send[k, 0, here, :] = jnp.concatenate(first, axis=0)
        raw_send[k, 1, here, :] = jnp.concatenate(last, axis=0)

    def first_split(g, _):
        first, last = [], []
        for j in range(8):
            value = b[g * 8 + j]
            put_split(g * 8 + j, value)
            first.append(value[:1])
            last.append(value[ny - 1 :])
        put_ends(0, g * 8, first, last)
        return 0

    lax.fori_loop(0, nx // 8, first_split, 0)

    def coefs(k, i):
        both = dot(split[flat(i), :], wc[...])
        c[k, inner(i), :] = both[:, :128] + both[:, 128:]

    def pack_y(k, i):
        seg = segments(step)
        base = pl.multiple_of(i * rows + ny, ny)
        first, second = (c[k, pl.ds(base + n, step, stride=ny), :] for n in (0, 1))
        last, before = (c[k, pl.ds(base + ny - n, step, stride=ny), :] for n in (1, 2))
        coef_send[k, pl.ds(pl.multiple_of(2 * ny + i * step, step), step), :] = jnp.where(
            seg == 3, pltpu.roll(second, 32, 1), first
        )
        coef_send[k, pl.ds(pl.multiple_of(2 * ny + nx + i * step, step), step), :] = jnp.where(
            seg == 2, pltpu.roll(before, 96, 1), last
        )

    def pack_x(k, side):
        seg = segments(ny)
        x, behind, where, turn = ((0, 1, 1, 32), (nx - 1, nx - 2, 0, 96))[side]
        own = c[k, cells(x), :]
        coef_send[k, pl.ds(side * ny, ny), :] = jnp.where(seg == where, pltpu.roll(c[k, cells(behind), :], turn, 1), own)
        if k < 2:
            corner_send[k, 2 * (1 - side)] = jnp.broadcast_to(own[ny - 1 :], (8, 128))
            corner_send[k, 2 * (1 - side) + 1] = jnp.broadcast_to(own[:1], (8, 128))

    fields = (b, v0)

    def x_copies(k, side):
        to = ((west, gy), (east, gy))[side]
        mine, theirs = side * ny, (1 - side) * ny
        pairs = [(coef_send.at[k, pl.ds(mine, ny)], coef_recv.at[k, pl.ds(theirs, ny)])]
        if k < 2:
            pairs.append((fields[k].at[(0, nx - 1)[side]], raw_recv.at[k, pl.ds(theirs, ny)]))
        copies = [
            pltpu.make_async_remote_copy(
                src_ref=src, dst_ref=dst, send_sem=xsend_sem.at[k, side, n], recv_sem=xrecv_sem.at[k, side, n],
                device_id=to, device_id_type=MESH,
            )
            for n, (src, dst) in enumerate(pairs)
        ]
        if k < 2:
            for n in (2 * (1 - side), 2 * (1 - side) + 1):
                copies.append(
                    pltpu.make_async_remote_copy(
                        src_ref=corner_send.at[k, n], dst_ref=corner_recv.at[k, n],
                        send_sem=ksend_sem.at[k, n], recv_sem=krecv_sem.at[k, n],
                        device_id=diagonals[n], device_id_type=MESH,
                    )
                )
        return copies

    def y_copies(k, side, i):
        count = nx if k == 0 else step
        here = pl.ds(pl.multiple_of(i * count, step), count)
        there = pl.ds(pl.multiple_of(2 * ny + side * nx + i * count, step), count)
        pairs = [(coef_send.at[k, there], coef_recv.at[k, there])]
        if k < 2:
            pairs.append((raw_send.at[k, side, here], raw_recv.at[k, there]))
        return [
            pltpu.make_async_remote_copy(
                src_ref=src, dst_ref=dst, send_sem=ysend_sem.at[k, side, n, i], recv_sem=yrecv_sem.at[k, side, n, i],
                device_id=(gx, (south, north)[side]), device_id_type=MESH,
            )
            for n, (src, dst) in enumerate(pairs)
        ]

    def send_chunk(k, turn, i):
        for side in (0, 1):

            @pl.when(turn == side)
            def _():
                pack_x(k, side)
                for copy in x_copies(k, side):
                    copy.start()

        pack_y(k, i)
        for side in (0, 1):
            for copy in y_copies(k, side, i):
                copy.start()

    def all_copies(k):
        return [copy for side in (0, 1) for copy in x_copies(k, side)] + [
            copy for side in (0, 1) for i in range(1 if k == 0 else chunks) for copy in y_copies(k, side, i)
        ]

    def chunk(turn):
        return jnp.where(turn == 0, 0, jnp.where(turn == 1, chunks - 1, turn - 1))

    def diagonal(out, place):
        def body(i, _):
            value = split[flat(i), :]
            out[place(i), :] = dot(jnp.concatenate([value, value[:, :nz]], axis=1), wb[...])
            return 0

        lax.fori_loop(0, chunks, body, 0)

    def couple(k, out, place, start=0, sums=None):
        seg = segments(ny)
        line = lax.broadcasted_iota(jnp.int32, (ny, 128), 0)
        use_after = (seg == 2) & (line < ny - 1)
        use_before = (seg == 3) & (line > 0)

        def body(i, carry):
            for j in range(step):
                x = i * step + j
                here = c[k, cells(x), :]
                coef = jnp.where(seg == 0, c[k, cells(x + 1), :], jnp.where(seg == 1, c[k, cells(x - 1), :], 0.0))
                coef = jnp.where(use_after, pltpu.roll(here, ny - 1, 0), coef)
                coef = jnp.where(use_before, pltpu.roll(here, 1, 0), coef)
                coef = coef * mask[pl.ds(pl.multiple_of(x * ny, ny), ny), :]
                high, low = halves(coef)
                dsplit[j * ny : (j + 1) * ny, 0:128] = high
                dsplit[j * ny : (j + 1) * ny, 128:256] = low
            value = dsplit[...]
            total = out[place(i), :] + dot(jnp.concatenate([value, value[:, :128]], axis=1), wd[...])
            out[place(i), :] = total
            if sums is not None:
                for j in range(step):
                    carry = sums(i * step + j, total[j * ny : (j + 1) * ny, :], carry)
            return carry

        return lax.fori_loop(0, chunks, body, start)

    def add_ends(out, at, first, last):
        line = lax.broadcasted_iota(jnp.int32, (8, nz), 0)
        for x in range(nx):
            head, tail = at + x * ny, at + x * ny + ny - 8
            more = jnp.broadcast_to(uy[first + x : first + x + 1, :], (8, nz))
            out[head : head + 8, :] = out[head : head + 8, :] + jnp.where(line == 0, more, 0.0)
            more = jnp.broadcast_to(uy[last + x : last + x + 1, :], (8, nz))
            out[tail : tail + 8, :] = out[tail : tail + 8, :] + jnp.where(line == 7, more, 0.0)

    def put_fix(at, value):
        high, low = halves(value)
        fsplit[at : at + value.shape[0], 0:128] = high
        fsplit[at : at + value.shape[0], 128:256] = low

    def fix_own(k):
        put_fix(0, coef_recv[k] * edge_mask[...])

    def fix_halo(k):
        got = lambda at, count: coef_recv[k, at : at + count, :]
        corner = lambda n, count: jnp.broadcast_to(corner_recv[k, n][:1], (count, 128))
        ws, wn, es, en = range(4)
        seg = segments(ny)
        line = lax.broadcasted_iota(jnp.int32, (ny, 128), 0)
        for side, (lo, hi) in enumerate(((ws, wn), (es, en))):
            here = got(side * ny, ny)
            after = jnp.where(line == ny - 1, corner(hi, ny), pltpu.roll(here, ny - 1, 0))
            before = jnp.where(line == 0, corner(lo, ny), pltpu.roll(here, 1, 0))
            if side == 0:
                ahead, behind = c[k, cells(0), :], pltpu.roll(here, 32, 1)
            else:
                ahead, behind = pltpu.roll(here, 96, 1), c[k, cells(nx - 1), :]
            coef = jnp.where(seg == 0, ahead, jnp.where(seg == 1, behind, jnp.where(seg == 2, after, before)))
            put_fix(edge + side * ny, coef * mask[lines + side * ny : lines + (side + 1) * ny, :])
        seg = segments(nx)
        line = lax.broadcasted_iota(jnp.int32, (nx, 128), 0)
        for side, (lo, hi) in enumerate(((wn, en), (ws, es))):
            at = 2 * ny + side * nx
            here = got(at, nx)
            ahead = jnp.where(line == nx - 1, corner(hi, nx), pltpu.roll(here, nx - 1, 0))
            behind = jnp.where(line == 0, corner(lo, nx), pltpu.roll(here, 1, 0))
            if side == 0:
                after = pltpu.roll(here, 96, 1)
                before = c[k, pl.ds(ny + ny - 1, nx, stride=ny), :]
            else:
                after = c[k, pl.ds(ny, nx, stride=ny), :]
                before = pltpu.roll(here, 32, 1)
            coef = jnp.where(seg == 0, ahead, jnp.where(seg == 1, behind, jnp.where(seg == 2, after, before)))
            put_fix(edge + at, coef * mask[lines + at : lines + at + nx, :])

    def finish_field(k, u):
        for copy in all_copies(k):
            copy.wait_recv()
        fix_own(k)
        fix_halo(k)
        high, low = halves(raw_recv[k])
        value = fsplit[...]
        more = dot(jnp.concatenate([value, value[:, :128]], axis=1), wd[...])
        halo = more[edge:] + dot(jnp.concatenate([high, low, high], axis=1), wb[...])
        u[0:ny, :] = halo[:ny]
        u[(nx + 1) * ny : (nx + 2) * ny, :] = halo[ny : 2 * ny]
        uy[0 : 2 * nx, :] = halo[2 * ny :]
        uy[2 * nx : 4 * nx, :] = more[2 * ny : edge]
        u[cells(0), :] = u[cells(0), :] + more[:ny]
        u[cells(nx - 1), :] = u[cells(nx - 1), :] + more[ny : 2 * ny]
        add_ends(u, ny, 3 * nx, 2 * nx)
        return more[:edge]

    zero = jnp.zeros((8, nz), F32)

    def operate(k, u, v, start, sums, after_chunk):
        top = lax.broadcasted_iota(jnp.int32, (8, nz), 0)

        def body(turn, carry):
            i = chunk(turn)

            for g in range(step // 8):
                first, last = [], []
                for j in range(8):
                    x = i * step + g * 8 + j
                    here = u[cells(x), :]
                    up, down = pltpu.roll(here, ny - 1, 0), pltpu.roll(here, 1, 0)
                    after = jnp.where(top == 7, jnp.broadcast_to(uy[pl.ds(x, 1), :], (8, nz)), up[ny - 8 :])
                    before = jnp.where(top == 0, jnp.broadcast_to(uy[pl.ds(nx + x, 1), :], (8, nz)), down[:8])
                    beside = jnp.concatenate([up[: ny - 8], after], axis=0) + jnp.concatenate([before, down[8:]], axis=0)
                    beside = beside + u[cells(x + 1), :] + u[cells(x - 1), :]
                    beside = beside + pltpu.roll(here, 1, 1) + pltpu.roll(here, nz - 1, 1)
                    value = (6.0 + mass_shift) * here - beside
                    v[x] = value
                    put_split(x, value)
                    first.append(value[:1])
                    last.append(value[ny - 1 :])
                    carry = sums(x, here, value, carry)
                if k < 2:
                    put_ends(k, i * step + g * 8, first, last)
            after_chunk(turn, i)
            return carry

        return lax.fori_loop(0, chunks, body, start)

    def coefs_and_send(k):
        def go(turn, i):
            coefs(k, i)
            send_chunk(k, turn, i)

        return go

    def first_coefs(i, _):
        coefs(0, i)
        pack_y(0, i)
        return 0

    lax.fori_loop(0, chunks, first_coefs, 0)
    for side in (0, 1):
        pack_x(0, side)

    pl.semaphore_wait(barrier, ndx + ndy + 2)
    for copy in all_copies(0):
        copy.start()

    loads[0].wait()
    high, low = halves(binv[...].T)
    wb[0:nz, :] = high
    wb[nz : 2 * nz, :] = high
    wb[2 * nz : 3 * nz, :] = low
    swapped = jnp.concatenate([bases[1], bases[0], bases[3], bases[2]], axis=0)
    high, low = halves(swapped)
    wd[0:128, :] = high
    wd[128:256, :] = high
    wd[256:384, :] = low

    for k in range(3):
        c[k, 0:ny, :] = jnp.zeros((ny, 128), F32)
        c[k, (nx + 1) * ny : (nx + 2) * ny, :] = jnp.zeros((ny, 128), F32)

    for load in loads[6:]:
        load.wait()
    tall = nx + 16
    lane = lax.broadcasted_iota(jnp.int32, (tall, 128), 1)
    offset = lax.rem(gy, per_tile) * ny - 32
    window = []
    for e in (0, 1):
        below, own, above = (pltpu.roll(tiles[e, side].astype(F32), lax.rem(128 - offset, 128), 1) for side in range(3))
        window.append(jnp.where(lane + offset < 0, below, jnp.where(lane + offset >= 128, above, own)))
    ranks_x, ranks_y = window
    ranks_behind = pltpu.roll(ranks_x, 1, 0)
    wide = jnp.where(
        lane < 32,
        pltpu.roll(ranks_x, 96, 1),
        jnp.where(lane < 64, ranks_behind, jnp.where(lane < 96, pltpu.roll(ranks_y, 32, 1), pltpu.roll(ranks_y, 65, 1))),
    )
    limits[...] = wide
    level = lambda count: lax.rem(lax.broadcasted_iota(jnp.int32, (count, 128), 1), 32).astype(F32)
    for side, y in enumerate((32 + ny, 31)):
        column = lambda table, t: jnp.broadcast_to(table[:, t : t + 1], (tall, 128))
        own_y, back_y = column(ranks_y, y), column(ranks_y, y - 1)
        limit = jnp.where(
            lane < 32,
            column(ranks_x, y),
            jnp.where(lane < 64, column(ranks_behind, y), jnp.where(lane < 96, own_y, back_y)),
        )
        at = lines + 2 * ny + side * nx
        mask[at : at + nx, :] = jnp.where(level(nx) < limit[8 : 8 + nx], 1.0, 0.0)
    own = lax.rem(lax.broadcasted_iota(jnp.int32, (ny, 128), 1), 32) == lax.broadcasted_iota(jnp.int32, (ny, 128), 0)
    spread = (
        lax.broadcasted_iota(jnp.int32, (128, 128), 0) // 32 == lax.broadcasted_iota(jnp.int32, (128, 128), 1) // 32
    ).astype(F32).astype(BF16)

    def place(x, at):
        line_ranks = jnp.broadcast_to(limits[pl.ds(x + 8, 1), :], (ny, 128))
        picks[pl.ds(pl.multiple_of(at * ny, ny), ny), :] = jnp.where(own, line_ranks, 0.0).astype(BF16)

    def place_own(x, _):
        place(x, x)
        return 0

    lax.fori_loop(0, nx, place_own, 0, unroll=4)
    place(-1, nx)
    place(nx, nx + 1)

    def fill_mask(i, _):
        mask[flat(i), :] = jnp.where(level(rows) < dot(picks[flat(i), :], spread), 1.0, 0.0)
        return 0

    lax.fori_loop(0, chunks, fill_mask, 0)
    mask[lines : lines + 2 * ny, :] = jnp.where(level(2 * ny) < dot(picks[lines : lines + 2 * ny, :], spread), 1.0, 0.0)
    edge_mask[0:ny, :] = jnp.where(segments(ny) == 1, mask[0:ny, :], 0.0)
    edge_mask[ny : 2 * ny, :] = jnp.where(segments(ny) == 0, mask[lines - ny : lines, :], 0.0)
    edge_mask[2 * ny : 2 * ny + nx, :] = jnp.where(segments(nx) == 2, mask[pl.ds(ny - 1, nx, stride=ny), :], 0.0)
    edge_mask[2 * ny + nx : edge, :] = jnp.where(segments(nx) == 3, mask[pl.ds(0, nx, stride=ny), :], 0.0)

    diagonal(u0, inner)
    couple(0, u0, inner)
    finish_field(0, u0)

    operate(1, u0, v0, 0, lambda x, here, value, carry: carry, coefs_and_send(1))

    diagonal(u1, inner)

    def early(x, total, carry):
        have = u0[cells(x), :]
        return (
            carry[0] + fold(have * b[x]), carry[1] + fold(have * v0[x]),
            carry[2] + fold(total * b[x]), carry[3] + fold(total * v0[x]),
        )

    bu0, u0v0, bu1, v0u1 = couple(1, u1, inner, (zero, zero, zero, zero), early)
    more = finish_field(1, u1)
    pieces = (
        (more[:ny], lambda k: fields[k][0]),
        (more[ny : 2 * ny], lambda k: fields[k][nx - 1]),
        (more[2 * ny : 2 * ny + nx], lambda k: raw_send[k, 1]),
        (more[2 * ny + nx :], lambda k: raw_send[k, 0]),
    )
    for piece, line_of in pieces:
        bu1 = bu1 + fold(piece * line_of(0))
        v0u1 = v0u1 + fold(piece * line_of(1))

    u1v1 = operate(
        2, u1, v1, zero, lambda x, here, value, carry: carry + fold(here * value), lambda turn, i: None
    )

    def row_of(value):
        value = value[:, :128] + value[:, 128:]
        return jnp.sum(value, axis=0, keepdims=True)

    partial = jnp.concatenate(
        [row_of(s) for s in (bu0, u0v0, bu1, v0u1, u1v1)] + [jnp.zeros((3, 128), F32)], axis=0
    )
    part[0] = partial
    got_y[gy] = partial
    along_y = [
        pltpu.make_async_remote_copy(
            src_ref=part.at[0], dst_ref=got_y.at[gy], send_sem=rsend_sem.at[0, k], recv_sem=rrecv_sem.at[0, k],
            device_id=(gx, lax.rem(gy + k, ndy)), device_id_type=MESH,
        )
        for k in range(1, ndy)
    ]
    for copy in along_y:
        copy.start()

    def last_send(turn, _):
        coefs_and_send(2)(turn, chunk(turn))
        return 0

    lax.fori_loop(0, chunks, last_send, 0)
    diagonal(u2, flat)
    couple(2, u2, flat)
    for copy in along_y:
        copy.wait()
    partial = jnp.sum(got_y[...], axis=0)
    part[1] = partial
    got_x[gx] = partial
    along_x = [
        pltpu.make_async_remote_copy(
            src_ref=part.at[1], dst_ref=got_x.at[gx], send_sem=rsend_sem.at[1, k], recv_sem=rrecv_sem.at[1, k],
            device_id=(lax.rem(gx + k, ndx), gy), device_id_type=MESH,
        )
        for k in range(1, ndx)
    ]
    for copy in along_x:
        copy.start()
    for copy in all_copies(2):
        copy.wait_recv()
    fix_own(2)
    value = fsplit[0:edge, :]
    more = dot(jnp.concatenate([value, value[:, :128]], axis=1), wd[...])
    uy[2 * nx : 4 * nx, :] = more[2 * ny :]
    u2[0:ny, :] = u2[0:ny, :] + more[:ny]
    u2[lines - ny : lines, :] = u2[lines - ny : lines, :] + more[ny : 2 * ny]
    add_ends(u2, 0, 3 * nx, 2 * nx)
    for k in range(3):
        for copy in all_copies(k):
            copy.wait_send()
    for copy in along_x:
        copy.wait()
    total = jnp.sum(jnp.sum(got_x[...], axis=0), axis=1, keepdims=True)
    s = [total[k : k + 1, :] for k in range(5)]

    alpha0 = s[S_BU0] / s[S_U0V0]
    rz1 = s[S_BU0] - alpha0 * (s[S_U0V0] + s[S_BU1]) + alpha0 * (alpha0 * s[S_V0U1])
    grow = 1.0 + rz1 / s[S_BU0]
    curve = grow * (grow * s[S_U0V0] - 2.0 * (alpha0 * s[S_V0U1])) + alpha0 * (alpha0 * s[S_U1V1])
    alpha1 = rz1 / curve
    on0 = alpha0 + alpha1 * grow
    on1 = -(alpha1 * alpha0)
    scale[0] = jnp.broadcast_to(on0, (8, 128))
    scale[1] = jnp.broadcast_to(on1, (8, 128))


def combine(b, u0, u1, u2, v0, v1, scale, x_any, gap_any, z_any, x_out, gap_out, z_out, sem):
    nx, ny, nz = x_out.shape
    step = 8
    on0, on1 = (jnp.concatenate([jnp.concatenate([scale[k]] * 2, axis=1)] * (ny // 8), axis=0) for k in (0, 1))

    def copies(i):
        here = pl.ds(pl.multiple_of(i * step, step), step)
        return [
            pltpu.make_async_copy(out.at[here], out_any.at[here], sem.at[n, i])
            for n, (out, out_any) in enumerate(((x_out, x_any), (z_out, z_any), (gap_out, gap_any)))
        ]

    def body(i, _):
        for j in range(step):
            x = i * step + j
            at = pl.ds(pl.multiple_of((x + 1) * ny, ny), ny)
            f0, f1 = u0[at, :], u1[at, :]
            x_out[x] = on0 * f0 + on1 * f1
            z_out[x] = f0 - on0 * f1 - on1 * u2[pl.ds(pl.multiple_of(x * ny, ny), ny), :]
            gap_out[x] = b[x] - on0 * v0[x] - on1 * v1[x]
        for copy in copies(i):
            copy.start()
        return 0

    lax.fori_loop(0, nx // step, body, 0)

    def finish(i, _):
        for copy in copies(i):
            copy.wait()
        return 0

    lax.fori_loop(0, nx // step, finish, 0)


def per_device(devs, right_side, block_inverse, basis_left, basis_right, ranks):
    nx, ny, nz = right_side.shape
    ndx, ndy = devs
    lines = nx * ny
    padded = lines + 2 * ny
    edge = 2 * (nx + ny)
    block = jax.ShapeDtypeStruct(right_side.shape, F32)
    framed = jax.ShapeDtypeStruct((padded, nz), F32)
    arrays = (right_side, block_inverse, basis_left, basis_right, ranks)
    fields = pl.pallas_call(
        functools.partial(kernel, devs),
        out_shape=(
            block, framed, framed, jax.ShapeDtypeStruct((lines, nz), F32), block, block,
            jax.ShapeDtypeStruct((2, 8, 128), F32),
        ),
        in_specs=[pl.BlockSpec(memory_space=pltpu.HBM)] * 5,
        out_specs=[pl.BlockSpec(memory_space=pltpu.VMEM)] * 7,
        scratch_shapes=[
            pltpu.VMEM((nz, nz), F32),
            pltpu.VMEM((4, 32, nz), F32),
            pltpu.VMEM((2, 3, nx + 16, 128), jnp.int32),
            pltpu.VMEM((nx + 16, 128), F32),
            pltpu.VMEM((lines + 2 * ny, 128), BF16),
            pltpu.VMEM((3 * nz, nz), BF16),
            pltpu.VMEM((2 * nz, 256), BF16),
            pltpu.VMEM((384, nz), BF16),
            pltpu.VMEM((lines + edge, 128), F32),
            pltpu.VMEM((edge, 128), F32),
            pltpu.VMEM((lines, 2 * nz), BF16),
            pltpu.VMEM((16 * ny, 256), BF16),
            pltpu.VMEM((2 * edge, 256), BF16),
            pltpu.VMEM((3, padded, 128), F32),
            pltpu.VMEM((3, edge, 128), F32),
            pltpu.VMEM((3, edge, 128), F32),
            pltpu.VMEM((2, 2, nx, nz), F32),
            pltpu.VMEM((2, edge, nz), F32),
            pltpu.VMEM((2, 4, 8, 128), F32),
            pltpu.VMEM((2, 4, 8, 128), F32),
            pltpu.VMEM((4 * nx, nz), F32),
            pltpu.VMEM((2, 8, 128), F32),
            pltpu.VMEM((ndy, 8, 128), F32),
            pltpu.VMEM((ndx, 8, 128), F32),
            pltpu.SemaphoreType.DMA((24,)),
            pltpu.SemaphoreType.DMA((3, 2, 2)),
            pltpu.SemaphoreType.DMA((3, 2, 2)),
            pltpu.SemaphoreType.DMA((3, 2, 2, nx // 16)),
            pltpu.SemaphoreType.DMA((3, 2, 2, nx // 16)),
            pltpu.SemaphoreType.DMA((2, 4)),
            pltpu.SemaphoreType.DMA((2, 4)),
            pltpu.SemaphoreType.DMA((2, ndy)),
            pltpu.SemaphoreType.DMA((2, ndy)),
        ],
        compiler_params=pltpu.CompilerParams(
            collective_id=0, has_side_effects=True, vmem_limit_bytes=32 * 1024 * 1024
        ),
    )(*(pltpu.with_memory_space_constraint(array, pltpu.HBM) for array in arrays))
    return pl.pallas_call(
        combine,
        out_shape=(block, block, block),
        in_specs=[pl.BlockSpec(memory_space=pltpu.VMEM)] * 7,
        out_specs=[pl.BlockSpec(memory_space=pltpu.HBM)] * 3,
        scratch_shapes=[pltpu.VMEM((nx, ny, nz), F32)] * 3 + [pltpu.SemaphoreType.DMA((3, nx // 8))],
        compiler_params=pltpu.CompilerParams(vmem_limit_bytes=32 * 1024 * 1024),
    )(*fields)


def solution(mesh):
    devs = (mesh.shape["gx"], mesh.shape["gy"])
    return jax.shard_map(
        functools.partial(per_device, devs),
        mesh=mesh,
        in_specs=(P("gx", "gy", None), P(), P(), P(), P()),
        out_specs=(P("gx", "gy", None),) * 3,
        check_vma=False,
    )
```

```python
import functools

import jax
import jax.numpy as jnp
from jax import lax
from jax.experimental import pallas as pl
from jax.experimental.pallas import tpu as pltpu
from jax.sharding import PartitionSpec as P

F32 = jnp.float32
BF16 = jnp.bfloat16
MESH = pl.DeviceIdType.MESH

mass_shift = 0.05

S_BU0, S_U0V0, S_BU1, S_V0U1, S_U1V1 = range(5)


def halves(value):
    high = value.astype(BF16)
    return high, (value - high.astype(F32)).astype(BF16)


def dot(a, b):
    return lax.dot_general(a, b, (((1,), (0,)), ((), ())), preferred_element_type=F32)


def fold(value):
    rows, width = value.shape
    return jnp.sum(value.reshape(rows // 8, 8, width), axis=0)


def kernel(
    devs, b_any, binv_any, left_any, right_any, ranks_any,
    b, u0, u1, u2, v0, v1, scale,
    binv, bases, tiles, limits, picks, wb, wc, wd, mask, edge_mask, split, dsplit, fsplit,
    c, coef_send, coef_recv, raw_send, raw_recv, corner_send, corner_recv, uy, part, got_y, got_x,
    load_sem, xsend_sem, xrecv_sem, ysend_sem, yrecv_sem, ksend_sem, krecv_sem, rsend_sem, rrecv_sem,
):
    ndx, ndy = devs
    nx, ny, nz = b.shape
    lines = nx * ny
    edge = 2 * ny + 2 * nx
    step = 16
    rows = step * ny
    chunks = nx // step
    gx = lax.axis_index("gx")
    gy = lax.axis_index("gy")
    east, west = lax.rem(gx + 1, ndx), lax.rem(gx + ndx - 1, ndx)
    north, south = lax.rem(gy + 1, ndy), lax.rem(gy + ndy - 1, ndy)
    diagonals = ((east, north), (east, south), (west, north), (west, south))

    per_tile = 128 // ny
    tile_count = ndy // per_tile
    tile = gy // per_tile
    row_starts = (
        (0, lax.rem(gx * nx + ndx * nx - 8, ndx * nx), 8),
        (8, gx * nx, nx),
        (8 + nx, lax.rem(gx * nx + nx, ndx * nx), 8),
    )
    loads = [
        pltpu.make_async_copy(binv_any.at[0], binv, load_sem.at[0]),
        pltpu.make_async_copy(right_any.at[0, 0], bases.at[0], load_sem.at[1]),
        pltpu.make_async_copy(left_any.at[0, 0], bases.at[1], load_sem.at[2]),
        pltpu.make_async_copy(right_any.at[1, 0], bases.at[2], load_sem.at[3]),
        pltpu.make_async_copy(left_any.at[1, 0], bases.at[3], load_sem.at[4]),
        pltpu.make_async_copy(b_any, b, load_sem.at[5]),
    ]
    for e in (0, 1):
        for side in (0, 1, 2):
            col = pl.multiple_of(lax.rem(tile + side + tile_count - 1, tile_count) * 128, 128)
            for to, start, count in row_starts:
                loads.append(
                    pltpu.make_async_copy(
                        ranks_any.at[e, 0, pl.ds(pl.multiple_of(start, 8), count), pl.ds(col, 128)],
                        tiles.at[e, side, pl.ds(to, count)],
                        load_sem.at[len(loads)],
                    )
                )
    for load in loads[1:6]:
        load.start()

    barrier = pltpu.get_barrier_semaphore()
    for k in range(1, ndy):
        pl.semaphore_signal(barrier, 1, device_id=(gx, lax.rem(gy + k, ndy)), device_id_type=MESH)
    for k in range(1, ndx):
        pl.semaphore_signal(barrier, 1, device_id=(lax.rem(gx + k, ndx), gy), device_id_type=MESH)
    for to in diagonals:
        pl.semaphore_signal(barrier, 1, device_id=to, device_id_type=MESH)

    for load in loads[:1] + loads[6:]:
        load.start()

    def cells(x):
        return pl.ds(pl.multiple_of((x + 1) * ny, ny), ny)

    def flat(i):
        return pl.ds(pl.multiple_of(i * rows, rows), rows)

    def inner(i):
        return pl.ds(pl.multiple_of(i * rows + ny, ny), rows)

    def segments(count):
        return lax.broadcasted_iota(jnp.int32, (count, 128), 1) // 32

    for load in loads[1:5]:
        load.wait()
    factors = bases[...].reshape(4 * 32, nz)
    high, low = halves(factors.T)
    wc[0:nz, 0:128] = high
    wc[0:nz, 128:256] = low
    wc[nz : 2 * nz, 0:128] = high
    wc[nz : 2 * nz, 128:256] = jnp.zeros((nz, 128), BF16)

    loads[5].wait()

    def put_split(x, value):
        at = pl.ds(pl.multiple_of(x * ny, ny), ny)
        high, low = halves(value)
        split[at, 0:nz] = high
        split[at, nz : 2 * nz] = low

    def put_ends(k, start, first, last):
        here = pl.ds(pl.multiple_of(start, 8), 8)
        raw_send[k, 0, here, :] = jnp.concatenate(first, axis=0)
        raw_send[k, 1, here, :] = jnp.concatenate(last, axis=0)

    def first_split(g, _):
        first, last = [], []
        for j in range(8):
            value = b[g * 8 + j]
            put_split(g * 8 + j, value)
            first.append(value[:1])
            last.append(value[ny - 1 :])
        put_ends(0, g * 8, first, last)
        return 0

    lax.fori_loop(0, nx // 8, first_split, 0)

    def coefs(k, i):
        both = dot(split[flat(i), :], wc[...])
        c[k, inner(i), :] = both[:, :128] + both[:, 128:]

    def pack_y(k, i):
        seg = segments(step)
        base = pl.multiple_of(i * rows + ny, ny)
        first, second = (c[k, pl.ds(base + n, step, stride=ny), :] for n in (0, 1))
        last, before = (c[k, pl.ds(base + ny - n, step, stride=ny), :] for n in (1, 2))
        coef_send[k, pl.ds(pl.multiple_of(2 * ny + i * step, step), step), :] = jnp.where(
            seg == 3, pltpu.roll(second, 32, 1), first
        )
        coef_send[k, pl.ds(pl.multiple_of(2 * ny + nx + i * step, step), step), :] = jnp.where(
            seg == 2, pltpu.roll(before, 96, 1), last
        )

    def pack_x(k, side):
        seg = segments(ny)
        x, behind, where, turn = ((0, 1, 1, 32), (nx - 1, nx - 2, 0, 96))[side]
        own = c[k, cells(x), :]
        coef_send[k, pl.ds(side * ny, ny), :] = jnp.where(seg == where, pltpu.roll(c[k, cells(behind), :], turn, 1), own)
        if k < 2:
            corner_send[k, 2 * (1 - side)] = jnp.broadcast_to(own[ny - 1 :], (8, 128))
            corner_send[k, 2 * (1 - side) + 1] = jnp.broadcast_to(own[:1], (8, 128))

    fields = (b, v0)

    def x_copies(k, side):
        to = ((west, gy), (east, gy))[side]
        mine, theirs = side * ny, (1 - side) * ny
        pairs = [(coef_send.at[k, pl.ds(mine, ny)], coef_recv.at[k, pl.ds(theirs, ny)])]
        if k < 2:
            pairs.append((fields[k].at[(0, nx - 1)[side]], raw_recv.at[k, pl.ds(theirs, ny)]))
        copies = [
            pltpu.make_async_remote_copy(
                src_ref=src, dst_ref=dst, send_sem=xsend_sem.at[k, side, n], recv_sem=xrecv_sem.at[k, side, n],
                device_id=to, device_id_type=MESH,
            )
            for n, (src, dst) in enumerate(pairs)
        ]
        if k < 2:
            for n in (2 * (1 - side), 2 * (1 - side) + 1):
                copies.append(
                    pltpu.make_async_remote_copy(
                        src_ref=corner_send.at[k, n], dst_ref=corner_recv.at[k, n],
                        send_sem=ksend_sem.at[k, n], recv_sem=krecv_sem.at[k, n],
                        device_id=diagonals[n], device_id_type=MESH,
                    )
                )
        return copies

    def y_copies(k, side, i):
        count = nx if k == 0 else step
        here = pl.ds(pl.multiple_of(i * count, step), count)
        there = pl.ds(pl.multiple_of(2 * ny + side * nx + i * count, step), count)
        pairs = [(coef_send.at[k, there], coef_recv.at[k, there])]
        if k < 2:
            pairs.append((raw_send.at[k, side, here], raw_recv.at[k, there]))
        return [
            pltpu.make_async_remote_copy(
                src_ref=src, dst_ref=dst, send_sem=ysend_sem.at[k, side, n, i], recv_sem=yrecv_sem.at[k, side, n, i],
                device_id=(gx, (south, north)[side]), device_id_type=MESH,
            )
            for n, (src, dst) in enumerate(pairs)
        ]

    def send_chunk(k, turn, i):
        for side in (0, 1):

            @pl.when(turn == side)
            def _():
                pack_x(k, side)
                for copy in x_copies(k, side):
                    copy.start()

        pack_y(k, i)
        for side in (0, 1):
            for copy in y_copies(k, side, i):
                copy.start()

    def all_copies(k):
        return [copy for side in (0, 1) for copy in x_copies(k, side)] + [
            copy for side in (0, 1) for i in range(1 if k == 0 else chunks) for copy in y_copies(k, side, i)
        ]

    def chunk(turn):
        return jnp.where(turn == 0, 0, jnp.where(turn == 1, chunks - 1, turn - 1))

    def diagonal(out, place):
        def body(i, _):
            value = split[flat(i), :]
            out[place(i), :] = dot(jnp.concatenate([value, value[:, :nz]], axis=1), wb[...])
            return 0

        lax.fori_loop(0, chunks, body, 0)

    def couple(k, out, place, start=0, sums=None):
        seg = segments(ny)
        line = lax.broadcasted_iota(jnp.int32, (ny, 128), 0)
        use_after = (seg == 2) & (line < ny - 1)
        use_before = (seg == 3) & (line > 0)

        def body(i, carry):
            for j in range(step):
                x = i * step + j
                here = c[k, cells(x), :]
                coef = jnp.where(seg == 0, c[k, cells(x + 1), :], jnp.where(seg == 1, c[k, cells(x - 1), :], 0.0))
                coef = jnp.where(use_after, pltpu.roll(here, ny - 1, 0), coef)
                coef = jnp.where(use_before, pltpu.roll(here, 1, 0), coef)
                coef = coef * mask[pl.ds(pl.multiple_of(x * ny, ny), ny), :]
                high, low = halves(coef)
                dsplit[j * ny : (j + 1) * ny, 0:128] = high
                dsplit[j * ny : (j + 1) * ny, 128:256] = low
            value = dsplit[...]
            total = out[place(i), :] + dot(jnp.concatenate([value, value[:, :128]], axis=1), wd[...])
            out[place(i), :] = total
            if sums is not None:
                for j in range(step):
                    carry = sums(i * step + j, total[j * ny : (j + 1) * ny, :], carry)
            return carry

        return lax.fori_loop(0, chunks, body, start)

    def add_ends(out, at, first, last):
        line = lax.broadcasted_iota(jnp.int32, (8, nz), 0)
        for x in range(nx):
            head, tail = at + x * ny, at + x * ny + ny - 8
            more = jnp.broadcast_to(uy[first + x : first + x + 1, :], (8, nz))
            out[head : head + 8, :] = out[head : head + 8, :] + jnp.where(line == 0, more, 0.0)
            more = jnp.broadcast_to(uy[last + x : last + x + 1, :], (8, nz))
            out[tail : tail + 8, :] = out[tail : tail + 8, :] + jnp.where(line == 7, more, 0.0)

    def put_fix(at, value):
        high, low = halves(value)
        fsplit[at : at + value.shape[0], 0:128] = high
        fsplit[at : at + value.shape[0], 128:256] = low

    def fix_own(k):
        put_fix(0, coef_recv[k] * edge_mask[...])

    def fix_halo(k):
        got = lambda at, count: coef_recv[k, at : at + count, :]
        corner = lambda n, count: jnp.broadcast_to(corner_recv[k, n][:1], (count, 128))
        ws, wn, es, en = range(4)
        seg = segments(ny)
        line = lax.broadcasted_iota(jnp.int32, (ny, 128), 0)
        for side, (lo, hi) in enumerate(((ws, wn), (es, en))):
            here = got(side * ny, ny)
            after = jnp.where(line == ny - 1, corner(hi, ny), pltpu.roll(here, ny - 1, 0))
            before = jnp.where(line == 0, corner(lo, ny), pltpu.roll(here, 1, 0))
            if side == 0:
                ahead, behind = c[k, cells(0), :], pltpu.roll(here, 32, 1)
            else:
                ahead, behind = pltpu.roll(here, 96, 1), c[k, cells(nx - 1), :]
            coef = jnp.where(seg == 0, ahead, jnp.where(seg == 1, behind, jnp.where(seg == 2, after, before)))
            put_fix(edge + side * ny, coef * mask[lines + side * ny : lines + (side + 1) * ny, :])
        seg = segments(nx)
        line = lax.broadcasted_iota(jnp.int32, (nx, 128), 0)
        for side, (lo, hi) in enumerate(((wn, en), (ws, es))):
            at = 2 * ny + side * nx
            here = got(at, nx)
            ahead = jnp.where(line == nx - 1, corner(hi, nx), pltpu.roll(here, nx - 1, 0))
            behind = jnp.where(line == 0, corner(lo, nx), pltpu.roll(here, 1, 0))
            if side == 0:
                after = pltpu.roll(here, 96, 1)
                before = c[k, pl.ds(ny + ny - 1, nx, stride=ny), :]
            else:
                after = c[k, pl.ds(ny, nx, stride=ny), :]
                before = pltpu.roll(here, 32, 1)
            coef = jnp.where(seg == 0, ahead, jnp.where(seg == 1, behind, jnp.where(seg == 2, after, before)))
            put_fix(edge + at, coef * mask[lines + at : lines + at + nx, :])

    def finish_field(k, u):
        for copy in all_copies(k):
            copy.wait_recv()
        fix_own(k)
        fix_halo(k)
        high, low = halves(raw_recv[k])
        value = fsplit[...]
        more = dot(jnp.concatenate([value, value[:, :128]], axis=1), wd[...])
        halo = more[edge:] + dot(jnp.concatenate([high, low, high], axis=1), wb[...])
        u[0:ny, :] = halo[:ny]
        u[(nx + 1) * ny : (nx + 2) * ny, :] = halo[ny : 2 * ny]
        uy[0 : 2 * nx, :] = halo[2 * ny :]
        uy[2 * nx : 4 * nx, :] = more[2 * ny : edge]
        u[cells(0), :] = u[cells(0), :] + more[:ny]
        u[cells(nx - 1), :] = u[cells(nx - 1), :] + more[ny : 2 * ny]
        add_ends(u, ny, 3 * nx, 2 * nx)
        return more[:edge]

    zero = jnp.zeros((8, nz), F32)

    def operate(k, u, v, start, sums, after_chunk):
        top = lax.broadcasted_iota(jnp.int32, (8, nz), 0)

        def body(turn, carry):
            i = chunk(turn)

            for g in range(step // 8):
                first, last = [], []
                for j in range(8):
                    x = i * step + g * 8 + j
                    here = u[cells(x), :]
                    up, down = pltpu.roll(here, ny - 1, 0), pltpu.roll(here, 1, 0)
                    after = jnp.where(top == 7, jnp.broadcast_to(uy[pl.ds(x, 1), :], (8, nz)), up[ny - 8 :])
                    before = jnp.where(top == 0, jnp.broadcast_to(uy[pl.ds(nx + x, 1), :], (8, nz)), down[:8])
                    beside = jnp.concatenate([up[: ny - 8], after], axis=0) + jnp.concatenate([before, down[8:]], axis=0)
                    beside = beside + u[cells(x + 1), :] + u[cells(x - 1), :]
                    beside = beside + pltpu.roll(here, 1, 1) + pltpu.roll(here, nz - 1, 1)
                    value = (6.0 + mass_shift) * here - beside
                    v[x] = value
                    put_split(x, value)
                    first.append(value[:1])
                    last.append(value[ny - 1 :])
                    carry = sums(x, here, value, carry)
                if k < 2:
                    put_ends(k, i * step + g * 8, first, last)
            after_chunk(turn, i)
            return carry

        return lax.fori_loop(0, chunks, body, start)

    def coefs_and_send(k):
        def go(turn, i):
            coefs(k, i)
            send_chunk(k, turn, i)

        return go

    def first_coefs(i, _):
        coefs(0, i)
        pack_y(0, i)
        return 0

    lax.fori_loop(0, chunks, first_coefs, 0)
    for side in (0, 1):
        pack_x(0, side)

    pl.semaphore_wait(barrier, ndx + ndy + 2)
    ends_x = [x_copies(0, side) for side in (0, 1)]
    for copy in ends_x[0][2:] + ends_x[1][2:] + y_copies(0, 0, 0) + y_copies(0, 1, 0) + ends_x[0][:2] + ends_x[1][:2]:
        copy.start()

    loads[0].wait()
    high, low = halves(binv[...].T)
    wb[0:nz, :] = high
    wb[nz : 2 * nz, :] = high
    wb[2 * nz : 3 * nz, :] = low
    swapped = jnp.concatenate([bases[1], bases[0], bases[3], bases[2]], axis=0)
    high, low = halves(swapped)
    wd[0:128, :] = high
    wd[128:256, :] = high
    wd[256:384, :] = low

    for k in range(3):
        c[k, 0:ny, :] = jnp.zeros((ny, 128), F32)
        c[k, (nx + 1) * ny : (nx + 2) * ny, :] = jnp.zeros((ny, 128), F32)

    for load in loads[6:]:
        load.wait()
    tall = nx + 16
    lane = lax.broadcasted_iota(jnp.int32, (tall, 128), 1)
    offset = lax.rem(gy, per_tile) * ny - 32
    window = []
    for e in (0, 1):
        below, own, above = (pltpu.roll(tiles[e, side].astype(F32), lax.rem(128 - offset, 128), 1) for side in range(3))
        window.append(jnp.where(lane + offset < 0, below, jnp.where(lane + offset >= 128, above, own)))
    ranks_x, ranks_y = window
    ranks_behind = pltpu.roll(ranks_x, 1, 0)
    wide = jnp.where(
        lane < 32,
        pltpu.roll(ranks_x, 96, 1),
        jnp.where(lane < 64, ranks_behind, jnp.where(lane < 96, pltpu.roll(ranks_y, 32, 1), pltpu.roll(ranks_y, 65, 1))),
    )
    limits[...] = wide
    level = lambda count: lax.rem(lax.broadcasted_iota(jnp.int32, (count, 128), 1), 32).astype(F32)
    for side, y in enumerate((32 + ny, 31)):
        column = lambda table, t: jnp.broadcast_to(table[:, t : t + 1], (tall, 128))
        own_y, back_y = column(ranks_y, y), column(ranks_y, y - 1)
        limit = jnp.where(
            lane < 32,
            column(ranks_x, y),
            jnp.where(lane < 64, column(ranks_behind, y), jnp.where(lane < 96, own_y, back_y)),
        )
        at = lines + 2 * ny + side * nx
        mask[at : at + nx, :] = jnp.where(level(nx) < limit[8 : 8 + nx], 1.0, 0.0)
    own = lax.rem(lax.broadcasted_iota(jnp.int32, (ny, 128), 1), 32) == lax.broadcasted_iota(jnp.int32, (ny, 128), 0)
    spread = (
        lax.broadcasted_iota(jnp.int32, (128, 128), 0) // 32 == lax.broadcasted_iota(jnp.int32, (128, 128), 1) // 32
    ).astype(F32).astype(BF16)

    def place(x, at):
        line_ranks = jnp.broadcast_to(limits[pl.ds(x + 8, 1), :], (ny, 128))
        picks[pl.ds(pl.multiple_of(at * ny, ny), ny), :] = jnp.where(own, line_ranks, 0.0).astype(BF16)

    def place_own(x, _):
        place(x, x)
        return 0

    lax.fori_loop(0, nx, place_own, 0, unroll=4)
    place(-1, nx)
    place(nx, nx + 1)

    def fill_mask(i, _):
        mask[flat(i), :] = jnp.where(level(rows) < dot(picks[flat(i), :], spread), 1.0, 0.0)
        return 0

    lax.fori_loop(0, chunks, fill_mask, 0)
    mask[lines : lines + 2 * ny, :] = jnp.where(level(2 * ny) < dot(picks[lines : lines + 2 * ny, :], spread), 1.0, 0.0)
    edge_mask[0:ny, :] = jnp.where(segments(ny) == 1, mask[0:ny, :], 0.0)
    edge_mask[ny : 2 * ny, :] = jnp.where(segments(ny) == 0, mask[lines - ny : lines, :], 0.0)
    edge_mask[2 * ny : 2 * ny + nx, :] = jnp.where(segments(nx) == 2, mask[pl.ds(ny - 1, nx, stride=ny), :], 0.0)
    edge_mask[2 * ny + nx : edge, :] = jnp.where(segments(nx) == 3, mask[pl.ds(0, nx, stride=ny), :], 0.0)

    diagonal(u0, inner)
    couple(0, u0, inner)
    finish_field(0, u0)

    operate(1, u0, v0, 0, lambda x, here, value, carry: carry, coefs_and_send(1))

    diagonal(u1, inner)

    def early(x, total, carry):
        have = u0[cells(x), :]
        return (
            carry[0] + fold(have * b[x]), carry[1] + fold(have * v0[x]),
            carry[2] + fold(total * b[x]), carry[3] + fold(total * v0[x]),
        )

    bu0, u0v0, bu1, v0u1 = couple(1, u1, inner, (zero, zero, zero, zero), early)
    more = finish_field(1, u1)
    pieces = (
        (more[:ny], lambda k: fields[k][0]),
        (more[ny : 2 * ny], lambda k: fields[k][nx - 1]),
        (more[2 * ny : 2 * ny + nx], lambda k: raw_send[k, 1]),
        (more[2 * ny + nx :], lambda k: raw_send[k, 0]),
    )
    for piece, line_of in pieces:
        bu1 = bu1 + fold(piece * line_of(0))
        v0u1 = v0u1 + fold(piece * line_of(1))

    u1v1 = operate(
        2, u1, v1, zero, lambda x, here, value, carry: carry + fold(here * value), lambda turn, i: None
    )

    def row_of(value):
        value = value[:, :128] + value[:, 128:]
        return jnp.sum(value, axis=0, keepdims=True)

    partial = jnp.concatenate(
        [row_of(s) for s in (bu0, u0v0, bu1, v0u1, u1v1)] + [jnp.zeros((3, 128), F32)], axis=0
    )
    part[0] = partial
    got_y[gy] = partial
    along_y = [
        pltpu.make_async_remote_copy(
            src_ref=part.at[0], dst_ref=got_y.at[gy], send_sem=rsend_sem.at[0, k], recv_sem=rrecv_sem.at[0, k],
            device_id=(gx, lax.rem(gy + k, ndy)), device_id_type=MESH,
        )
        for k in range(1, ndy)
    ]
    for copy in along_y:
        copy.start()

    def last_send(turn, _):
        coefs_and_send(2)(turn, chunk(turn))
        return 0

    lax.fori_loop(0, chunks, last_send, 0)
    diagonal(u2, flat)
    couple(2, u2, flat)
    for copy in along_y:
        copy.wait()
    partial = jnp.sum(got_y[...], axis=0)
    part[1] = partial
    got_x[gx] = partial
    along_x = [
        pltpu.make_async_remote_copy(
            src_ref=part.at[1], dst_ref=got_x.at[gx], send_sem=rsend_sem.at[1, k], recv_sem=rrecv_sem.at[1, k],
            device_id=(lax.rem(gx + k, ndx), gy), device_id_type=MESH,
        )
        for k in range(1, ndx)
    ]
    for copy in along_x:
        copy.start()
    for copy in all_copies(2):
        copy.wait_recv()
    fix_own(2)
    value = fsplit[0:edge, :]
    more = dot(jnp.concatenate([value, value[:, :128]], axis=1), wd[...])
    uy[2 * nx : 4 * nx, :] = more[2 * ny :]
    u2[0:ny, :] = u2[0:ny, :] + more[:ny]
    u2[lines - ny : lines, :] = u2[lines - ny : lines, :] + more[ny : 2 * ny]
    add_ends(u2, 0, 3 * nx, 2 * nx)
    for k in range(3):
        for copy in all_copies(k):
            copy.wait_send()
    for copy in along_x:
        copy.wait()
    total = jnp.sum(jnp.sum(got_x[...], axis=0), axis=1, keepdims=True)
    s = [total[k : k + 1, :] for k in range(5)]

    alpha0 = s[S_BU0] / s[S_U0V0]
    rz1 = s[S_BU0] - alpha0 * (s[S_U0V0] + s[S_BU1]) + alpha0 * (alpha0 * s[S_V0U1])
    grow = 1.0 + rz1 / s[S_BU0]
    curve = grow * (grow * s[S_U0V0] - 2.0 * (alpha0 * s[S_V0U1])) + alpha0 * (alpha0 * s[S_U1V1])
    alpha1 = rz1 / curve
    on0 = alpha0 + alpha1 * grow
    on1 = -(alpha1 * alpha0)
    scale[0] = jnp.broadcast_to(on0, (8, 128))
    scale[1] = jnp.broadcast_to(on1, (8, 128))


def combine(b, u0, u1, u2, v0, v1, scale, x_any, gap_any, z_any, x_out, gap_out, z_out, sem):
    nx, ny, nz = x_out.shape
    step = 8
    on0, on1 = (jnp.concatenate([jnp.concatenate([scale[k]] * 2, axis=1)] * (ny // 8), axis=0) for k in (0, 1))

    def copies(i):
        here = pl.ds(pl.multiple_of(i * step, step), step)
        return [
            pltpu.make_async_copy(out.at[here], out_any.at[here], sem.at[n, i])
            for n, (out, out_any) in enumerate(((x_out, x_any), (z_out, z_any), (gap_out, gap_any)))
        ]

    def body(i, _):
        for j in range(step):
            x = i * step + j
            at = pl.ds(pl.multiple_of((x + 1) * ny, ny), ny)
            f0, f1 = u0[at, :], u1[at, :]
            x_out[x] = on0 * f0 + on1 * f1
            z_out[x] = f0 - on0 * f1 - on1 * u2[pl.ds(pl.multiple_of(x * ny, ny), ny), :]
            gap_out[x] = b[x] - on0 * v0[x] - on1 * v1[x]
        for copy in copies(i):
            copy.start()
        return 0

    lax.fori_loop(0, nx // step, body, 0)

    def finish(i, _):
        for copy in copies(i):
            copy.wait()
        return 0

    lax.fori_loop(0, nx // step, finish, 0)


def per_device(devs, right_side, block_inverse, basis_left, basis_right, ranks):
    nx, ny, nz = right_side.shape
    ndx, ndy = devs
    lines = nx * ny
    padded = lines + 2 * ny
    edge = 2 * (nx + ny)
    block = jax.ShapeDtypeStruct(right_side.shape, F32)
    framed = jax.ShapeDtypeStruct((padded, nz), F32)
    arrays = (right_side, block_inverse, basis_left, basis_right, ranks)
    fields = pl.pallas_call(
        functools.partial(kernel, devs),
        out_shape=(
            block, framed, framed, jax.ShapeDtypeStruct((lines, nz), F32), block, block,
            jax.ShapeDtypeStruct((2, 8, 128), F32),
        ),
        in_specs=[pl.BlockSpec(memory_space=pltpu.HBM)] * 5,
        out_specs=[pl.BlockSpec(memory_space=pltpu.VMEM)] * 7,
        scratch_shapes=[
            pltpu.VMEM((nz, nz), F32),
            pltpu.VMEM((4, 32, nz), F32),
            pltpu.VMEM((2, 3, nx + 16, 128), jnp.int32),
            pltpu.VMEM((nx + 16, 128), F32),
            pltpu.VMEM((lines + 2 * ny, 128), BF16),
            pltpu.VMEM((3 * nz, nz), BF16),
            pltpu.VMEM((2 * nz, 256), BF16),
            pltpu.VMEM((384, nz), BF16),
            pltpu.VMEM((lines + edge, 128), F32),
            pltpu.VMEM((edge, 128), F32),
            pltpu.VMEM((lines, 2 * nz), BF16),
            pltpu.VMEM((16 * ny, 256), BF16),
            pltpu.VMEM((2 * edge, 256), BF16),
            pltpu.VMEM((3, padded, 128), F32),
            pltpu.VMEM((3, edge, 128), F32),
            pltpu.VMEM((3, edge, 128), F32),
            pltpu.VMEM((2, 2, nx, nz), F32),
            pltpu.VMEM((2, edge, nz), F32),
            pltpu.VMEM((2, 4, 8, 128), F32),
            pltpu.VMEM((2, 4, 8, 128), F32),
            pltpu.VMEM((4 * nx, nz), F32),
            pltpu.VMEM((2, 8, 128), F32),
            pltpu.VMEM((ndy, 8, 128), F32),
            pltpu.VMEM((ndx, 8, 128), F32),
            pltpu.SemaphoreType.DMA((24,)),
            pltpu.SemaphoreType.DMA((3, 2, 2)),
            pltpu.SemaphoreType.DMA((3, 2, 2)),
            pltpu.SemaphoreType.DMA((3, 2, 2, nx // 16)),
            pltpu.SemaphoreType.DMA((3, 2, 2, nx // 16)),
            pltpu.SemaphoreType.DMA((2, 4)),
            pltpu.SemaphoreType.DMA((2, 4)),
            pltpu.SemaphoreType.DMA((2, ndy)),
            pltpu.SemaphoreType.DMA((2, ndy)),
        ],
        compiler_params=pltpu.CompilerParams(
            collective_id=0, has_side_effects=True, vmem_limit_bytes=32 * 1024 * 1024
        ),
    )(*(pltpu.with_memory_space_constraint(array, pltpu.HBM) for array in arrays))
    return pl.pallas_call(
        combine,
        out_shape=(block, block, block),
        in_specs=[pl.BlockSpec(memory_space=pltpu.VMEM)] * 7,
        out_specs=[pl.BlockSpec(memory_space=pltpu.HBM)] * 3,
        scratch_shapes=[pltpu.VMEM((nx, ny, nz), F32)] * 3 + [pltpu.SemaphoreType.DMA((3, nx // 8))],
        compiler_params=pltpu.CompilerParams(vmem_limit_bytes=32 * 1024 * 1024),
    )(*fields)


def solution(mesh):
    devs = (mesh.shape["gx"], mesh.shape["gy"])
    return jax.shard_map(
        functools.partial(per_device, devs),
        mesh=mesh,
        in_specs=(P("gx", "gy", None), P(), P(), P(), P()),
        out_specs=(P("gx", "gy", None),) * 3,
        check_vma=False,
    )
```

```python
import functools

import jax
import jax.numpy as jnp
from jax import lax
from jax.experimental import pallas as pl
from jax.experimental.pallas import tpu as pltpu
from jax.sharding import PartitionSpec as P

F32 = jnp.float32
BF16 = jnp.bfloat16
MESH = pl.DeviceIdType.MESH

mass_shift = 0.05

S_BU0, S_U0V0, S_BU1, S_V0U1, S_U1V1 = range(5)


def halves(value):
    high = value.astype(BF16)
    return high, (value - high.astype(F32)).astype(BF16)


def dot(a, b):
    return lax.dot_general(a, b, (((1,), (0,)), ((), ())), preferred_element_type=F32)


def fold(value):
    rows, width = value.shape
    return jnp.sum(value.reshape(rows // 8, 8, width), axis=0)


def kernel(
    devs, b_any, binv_any, left_any, right_any, ranks_any,
    b, u0, u1, u2, v0, v1, scale,
    binv, bases, tiles, limits, picks, wb, wc, wd, mask, edge_mask, split, dsplit, fsplit,
    c, coef_send, coef_recv, raw_send, raw_recv, corner_send, corner_recv, uy, part, got_y, got_x,
    load_sem, xsend_sem, xrecv_sem, ysend_sem, yrecv_sem, ksend_sem, krecv_sem, rsend_sem, rrecv_sem,
):
    ndx, ndy = devs
    nx, ny, nz = b.shape
    lines = nx * ny
    edge = 2 * ny + 2 * nx
    step = 16
    rows = step * ny
    chunks = nx // step
    gx = lax.axis_index("gx")
    gy = lax.axis_index("gy")
    east, west = lax.rem(gx + 1, ndx), lax.rem(gx + ndx - 1, ndx)
    north, south = lax.rem(gy + 1, ndy), lax.rem(gy + ndy - 1, ndy)
    diagonals = ((east, north), (east, south), (west, north), (west, south))

    per_tile = 128 // ny
    tile_count = ndy // per_tile
    tile = gy // per_tile
    row_starts = (
        (0, lax.rem(gx * nx + ndx * nx - 8, ndx * nx), 8),
        (8, gx * nx, nx),
        (8 + nx, lax.rem(gx * nx + nx, ndx * nx), 8),
    )
    loads = [
        pltpu.make_async_copy(binv_any.at[0], binv, load_sem.at[0]),
        pltpu.make_async_copy(right_any.at[0, 0], bases.at[0], load_sem.at[1]),
        pltpu.make_async_copy(left_any.at[0, 0], bases.at[1], load_sem.at[2]),
        pltpu.make_async_copy(right_any.at[1, 0], bases.at[2], load_sem.at[3]),
        pltpu.make_async_copy(left_any.at[1, 0], bases.at[3], load_sem.at[4]),
        pltpu.make_async_copy(b_any, b, load_sem.at[5]),
    ]
    for e in (0, 1):
        for side in (0, 1, 2):
            col = pl.multiple_of(lax.rem(tile + side + tile_count - 1, tile_count) * 128, 128)
            for to, start, count in row_starts:
                loads.append(
                    pltpu.make_async_copy(
                        ranks_any.at[e, 0, pl.ds(pl.multiple_of(start, 8), count), pl.ds(col, 128)],
                        tiles.at[e, side, pl.ds(to, count)],
                        load_sem.at[len(loads)],
                    )
                )
    for load in loads[1:6]:
        load.start()

    barrier = pltpu.get_barrier_semaphore()
    for k in range(1, ndy):
        pl.semaphore_signal(barrier, 1, device_id=(gx, lax.rem(gy + k, ndy)), device_id_type=MESH)
    for k in range(1, ndx):
        pl.semaphore_signal(barrier, 1, device_id=(lax.rem(gx + k, ndx), gy), device_id_type=MESH)
    for to in diagonals:
        pl.semaphore_signal(barrier, 1, device_id=to, device_id_type=MESH)

    for load in loads[:1] + loads[6:]:
        load.start()

    def cells(x):
        return pl.ds(pl.multiple_of((x + 1) * ny, ny), ny)

    def flat(i):
        return pl.ds(pl.multiple_of(i * rows, rows), rows)

    def inner(i):
        return pl.ds(pl.multiple_of(i * rows + ny, ny), rows)

    def segments(count):
        return lax.broadcasted_iota(jnp.int32, (count, 128), 1) // 32

    for load in loads[1:5]:
        load.wait()
    factors = bases[...].reshape(4 * 32, nz)
    high, low = halves(factors.T)
    wc[0:nz, 0:128] = high
    wc[0:nz, 128:256] = low
    wc[nz : 2 * nz, 0:128] = high
    wc[nz : 2 * nz, 128:256] = jnp.zeros((nz, 128), BF16)

    loads[5].wait()

    def put_split(x, value):
        at = pl.ds(pl.multiple_of(x * ny, ny), ny)
        high, low = halves(value)
        split[at, 0:nz] = high
        split[at, nz : 2 * nz] = low

    def put_ends(k, start, first, last):
        here = pl.ds(pl.multiple_of(start, 8), 8)
        raw_send[k, 0, here, :] = jnp.concatenate(first, axis=0)
        raw_send[k, 1, here, :] = jnp.concatenate(last, axis=0)

    def first_split(g, _):
        first, last = [], []
        for j in range(8):
            value = b[g * 8 + j]
            put_split(g * 8 + j, value)
            first.append(value[:1])
            last.append(value[ny - 1 :])
        put_ends(0, g * 8, first, last)
        return 0

    lax.fori_loop(0, nx // 8, first_split, 0)

    def coefs(k, i):
        both = dot(split[flat(i), :], wc[...])
        c[k, inner(i), :] = both[:, :128] + both[:, 128:]

    def pack_y(k, i):
        seg = segments(step)
        base = pl.multiple_of(i * rows + ny, ny)
        first, second = (c[k, pl.ds(base + n, step, stride=ny), :] for n in (0, 1))
        last, before = (c[k, pl.ds(base + ny - n, step, stride=ny), :] for n in (1, 2))
        coef_send[k, pl.ds(pl.multiple_of(2 * ny + i * step, step), step), :] = jnp.where(
            seg == 3, pltpu.roll(second, 32, 1), first
        )
        coef_send[k, pl.ds(pl.multiple_of(2 * ny + nx + i * step, step), step), :] = jnp.where(
            seg == 2, pltpu.roll(before, 96, 1), last
        )

    def pack_x(k, side):
        seg = segments(ny)
        x, behind, where, turn = ((0, 1, 1, 32), (nx - 1, nx - 2, 0, 96))[side]
        own = c[k, cells(x), :]
        coef_send[k, pl.ds(side * ny, ny), :] = jnp.where(seg == where, pltpu.roll(c[k, cells(behind), :], turn, 1), own)
        if k < 2:
            corner_send[k, 2 * (1 - side)] = jnp.broadcast_to(own[ny - 1 :], (8, 128))
            corner_send[k, 2 * (1 - side) + 1] = jnp.broadcast_to(own[:1], (8, 128))

    fields = (b, v0)

    def x_copies(k, side):
        to = ((west, gy), (east, gy))[side]
        mine, theirs = side * ny, (1 - side) * ny
        pairs = [(coef_send.at[k, pl.ds(mine, ny)], coef_recv.at[k, pl.ds(theirs, ny)])]
        if k < 2:
            pairs.append((fields[k].at[(0, nx - 1)[side]], raw_recv.at[k, pl.ds(theirs, ny)]))
        copies = [
            pltpu.make_async_remote_copy(
                src_ref=src, dst_ref=dst, send_sem=xsend_sem.at[k, side, n], recv_sem=xrecv_sem.at[k, side, n],
                device_id=to, device_id_type=MESH,
            )
            for n, (src, dst) in enumerate(pairs)
        ]
        if k < 2:
            for n in (2 * (1 - side), 2 * (1 - side) + 1):
                copies.append(
                    pltpu.make_async_remote_copy(
                        src_ref=corner_send.at[k, n], dst_ref=corner_recv.at[k, n],
                        send_sem=ksend_sem.at[k, n], recv_sem=krecv_sem.at[k, n],
                        device_id=diagonals[n], device_id_type=MESH,
                    )
                )
        return copies

    def y_copies(k, side, i):
        count = nx if k == 0 else step
        here = pl.ds(pl.multiple_of(i * count, step), count)
        there = pl.ds(pl.multiple_of(2 * ny + side * nx + i * count, step), count)
        pairs = [(coef_send.at[k, there], coef_recv.at[k, there])]
        if k < 2:
            pairs.append((raw_send.at[k, side, here], raw_recv.at[k, there]))
        return [
            pltpu.make_async_remote_copy(
                src_ref=src, dst_ref=dst, send_sem=ysend_sem.at[k, side, n, i], recv_sem=yrecv_sem.at[k, side, n, i],
                device_id=(gx, (south, north)[side]), device_id_type=MESH,
            )
            for n, (src, dst) in enumerate(pairs)
        ]

    def send_chunk(k, turn, i):
        for side in (0, 1):

            @pl.when(turn == side)
            def _():
                pack_x(k, side)
                copies = x_copies(k, side)
                for copy in copies[2:] + copies[:2]:
                    copy.start()

        pack_y(k, i)
        for side in (0, 1):
            for copy in y_copies(k, side, i):
                copy.start()

    def all_copies(k):
        return [copy for side in (0, 1) for copy in x_copies(k, side)] + [
            copy for side in (0, 1) for i in range(1 if k == 0 else chunks) for copy in y_copies(k, side, i)
        ]

    def chunk(turn):
        return jnp.where(turn == 0, 0, jnp.where(turn == 1, chunks - 1, turn - 1))

    def diagonal(out, place):
        def body(i, _):
            value = split[flat(i), :]
            out[place(i), :] = dot(jnp.concatenate([value, value[:, :nz]], axis=1), wb[...])
            return 0

        lax.fori_loop(0, chunks, body, 0)

    def couple(k, out, place, start=0, sums=None):
        seg = segments(ny)
        line = lax.broadcasted_iota(jnp.int32, (ny, 128), 0)
        use_after = (seg == 2) & (line < ny - 1)
        use_before = (seg == 3) & (line > 0)

        def body(i, carry):
            for j in range(step):
                x = i * step + j
                here = c[k, cells(x), :]
                coef = jnp.where(seg == 0, c[k, cells(x + 1), :], jnp.where(seg == 1, c[k, cells(x - 1), :], 0.0))
                coef = jnp.where(use_after, pltpu.roll(here, ny - 1, 0), coef)
                coef = jnp.where(use_before, pltpu.roll(here, 1, 0), coef)
                coef = coef * mask[pl.ds(pl.multiple_of(x * ny, ny), ny), :]
                high, low = halves(coef)
                dsplit[j * ny : (j + 1) * ny, 0:128] = high
                dsplit[j * ny : (j + 1) * ny, 128:256] = low
            value = dsplit[...]
            total = out[place(i), :] + dot(jnp.concatenate([value, value[:, :128]], axis=1), wd[...])
            out[place(i), :] = total
            if sums is not None:
                for j in range(step):
                    carry = sums(i * step + j, total[j * ny : (j + 1) * ny, :], carry)
            return carry

        return lax.fori_loop(0, chunks, body, start)

    def add_ends(out, at, first, last):
        line = lax.broadcasted_iota(jnp.int32, (8, nz), 0)
        for x in range(nx):
            head, tail = at + x * ny, at + x * ny + ny - 8
            more = jnp.broadcast_to(uy[first + x : first + x + 1, :], (8, nz))
            out[head : head + 8, :] = out[head : head + 8, :] + jnp.where(line == 0, more, 0.0)
            more = jnp.broadcast_to(uy[last + x : last + x + 1, :], (8, nz))
            out[tail : tail + 8, :] = out[tail : tail + 8, :] + jnp.where(line == 7, more, 0.0)

    def put_fix(at, value):
        high, low = halves(value)
        fsplit[at : at + value.shape[0], 0:128] = high
        fsplit[at : at + value.shape[0], 128:256] = low

    def fix_own(k):
        put_fix(0, coef_recv[k] * edge_mask[...])

    def fix_halo(k):
        got = lambda at, count: coef_recv[k, at : at + count, :]
        corner = lambda n, count: jnp.broadcast_to(corner_recv[k, n][:1], (count, 128))
        ws, wn, es, en = range(4)
        seg = segments(ny)
        line = lax.broadcasted_iota(jnp.int32, (ny, 128), 0)
        for side, (lo, hi) in enumerate(((ws, wn), (es, en))):
            here = got(side * ny, ny)
            after = jnp.where(line == ny - 1, corner(hi, ny), pltpu.roll(here, ny - 1, 0))
            before = jnp.where(line == 0, corner(lo, ny), pltpu.roll(here, 1, 0))
            if side == 0:
                ahead, behind = c[k, cells(0), :], pltpu.roll(here, 32, 1)
            else:
                ahead, behind = pltpu.roll(here, 96, 1), c[k, cells(nx - 1), :]
            coef = jnp.where(seg == 0, ahead, jnp.where(seg == 1, behind, jnp.where(seg == 2, after, before)))
            put_fix(edge + side * ny, coef * mask[lines + side * ny : lines + (side + 1) * ny, :])
        seg = segments(nx)
        line = lax.broadcasted_iota(jnp.int32, (nx, 128), 0)
        for side, (lo, hi) in enumerate(((wn, en), (ws, es))):
            at = 2 * ny + side * nx
            here = got(at, nx)
            ahead = jnp.where(line == nx - 1, corner(hi, nx), pltpu.roll(here, nx - 1, 0))
            behind = jnp.where(line == 0, corner(lo, nx), pltpu.roll(here, 1, 0))
            if side == 0:
                after = pltpu.roll(here, 96, 1)
                before = c[k, pl.ds(ny + ny - 1, nx, stride=ny), :]
            else:
                after = c[k, pl.ds(ny, nx, stride=ny), :]
                before = pltpu.roll(here, 32, 1)
            coef = jnp.where(seg == 0, ahead, jnp.where(seg == 1, behind, jnp.where(seg == 2, after, before)))
            put_fix(edge + at, coef * mask[lines + at : lines + at + nx, :])

    def finish_field(k, u):
        for copy in all_copies(k):
            copy.wait_recv()
        fix_own(k)
        fix_halo(k)
        high, low = halves(raw_recv[k])
        value = fsplit[...]
        more = dot(jnp.concatenate([value, value[:, :128]], axis=1), wd[...])
        halo = more[edge:] + dot(jnp.concatenate([high, low, high], axis=1), wb[...])
        u[0:ny, :] = halo[:ny]
        u[(nx + 1) * ny : (nx + 2) * ny, :] = halo[ny : 2 * ny]
        uy[0 : 2 * nx, :] = halo[2 * ny :]
        uy[2 * nx : 4 * nx, :] = more[2 * ny : edge]
        u[cells(0), :] = u[cells(0), :] + more[:ny]
        u[cells(nx - 1), :] = u[cells(nx - 1), :] + more[ny : 2 * ny]
        add_ends(u, ny, 3 * nx, 2 * nx)
        return more[:edge]

    zero = jnp.zeros((8, nz), F32)

    def operate(k, u, v, start, sums, after_chunk):
        top = lax.broadcasted_iota(jnp.int32, (8, nz), 0)

        def body(turn, carry):
            i = chunk(turn)

            for g in range(step // 8):
                first, last = [], []
                for j in range(8):
                    x = i * step + g * 8 + j
                    here = u[cells(x), :]
                    up, down = pltpu.roll(here, ny - 1, 0), pltpu.roll(here, 1, 0)
                    after = jnp.where(top == 7, jnp.broadcast_to(uy[pl.ds(x, 1), :], (8, nz)), up[ny - 8 :])
                    before = jnp.where(top == 0, jnp.broadcast_to(uy[pl.ds(nx + x, 1), :], (8, nz)), down[:8])
                    beside = jnp.concatenate([up[: ny - 8], after], axis=0) + jnp.concatenate([before, down[8:]], axis=0)
                    beside = beside + u[cells(x + 1), :] + u[cells(x - 1), :]
                    beside = beside + pltpu.roll(here, 1, 1) + pltpu.roll(here, nz - 1, 1)
                    value = (6.0 + mass_shift) * here - beside
                    v[x] = value
                    put_split(x, value)
                    first.append(value[:1])
                    last.append(value[ny - 1 :])
                    carry = sums(x, here, value, carry)
                if k < 2:
                    put_ends(k, i * step + g * 8, first, last)
            after_chunk(turn, i)
            return carry

        return lax.fori_loop(0, chunks, body, start)

    def coefs_and_send(k):
        def go(turn, i):
            coefs(k, i)
            send_chunk(k, turn, i)

        return go

    def first_coefs(i, _):
        coefs(0, i)
        pack_y(0, i)
        return 0

    lax.fori_loop(0, chunks, first_coefs, 0)
    for side in (0, 1):
        pack_x(0, side)

    pl.semaphore_wait(barrier, ndx + ndy + 2)
    ends_x = [x_copies(0, side) for side in (0, 1)]
    for copy in ends_x[0][2:] + ends_x[1][2:] + y_copies(0, 0, 0) + y_copies(0, 1, 0) + ends_x[0][:2] + ends_x[1][:2]:
        copy.start()

    loads[0].wait()
    high, low = halves(binv[...].T)
    wb[0:nz, :] = high
    wb[nz : 2 * nz, :] = high
    wb[2 * nz : 3 * nz, :] = low
    swapped = jnp.concatenate([bases[1], bases[0], bases[3], bases[2]], axis=0)
    high, low = halves(swapped)
    wd[0:128, :] = high
    wd[128:256, :] = high
    wd[256:384, :] = low

    for k in range(3):
        c[k, 0:ny, :] = jnp.zeros((ny, 128), F32)
        c[k, (nx + 1) * ny : (nx + 2) * ny, :] = jnp.zeros((ny, 128), F32)

    for load in loads[6:]:
        load.wait()
    tall = nx + 16
    lane = lax.broadcasted_iota(jnp.int32, (tall, 128), 1)
    offset = lax.rem(gy, per_tile) * ny - 32
    window = []
    for e in (0, 1):
        below, own, above = (pltpu.roll(tiles[e, side].astype(F32), lax.rem(128 - offset, 128), 1) for side in range(3))
        window.append(jnp.where(lane + offset < 0, below, jnp.where(lane + offset >= 128, above, own)))
    ranks_x, ranks_y = window
    ranks_behind = pltpu.roll(ranks_x, 1, 0)
    wide = jnp.where(
        lane < 32,
        pltpu.roll(ranks_x, 96, 1),
        jnp.where(lane < 64, ranks_behind, jnp.where(lane < 96, pltpu.roll(ranks_y, 32, 1), pltpu.roll(ranks_y, 65, 1))),
    )
    limits[...] = wide
    level = lambda count: lax.rem(lax.broadcasted_iota(jnp.int32, (count, 128), 1), 32).astype(F32)
    for side, y in enumerate((32 + ny, 31)):
        column = lambda table, t: jnp.broadcast_to(table[:, t : t + 1], (tall, 128))
        own_y, back_y = column(ranks_y, y), column(ranks_y, y - 1)
        limit = jnp.where(
            lane < 32,
            column(ranks_x, y),
            jnp.where(lane < 64, column(ranks_behind, y), jnp.where(lane < 96, own_y, back_y)),
        )
        at = lines + 2 * ny + side * nx
        mask[at : at + nx, :] = jnp.where(level(nx) < limit[8 : 8 + nx], 1.0, 0.0)
    own = lax.rem(lax.broadcasted_iota(jnp.int32, (ny, 128), 1), 32) == lax.broadcasted_iota(jnp.int32, (ny, 128), 0)
    spread = (
        lax.broadcasted_iota(jnp.int32, (128, 128), 0) // 32 == lax.broadcasted_iota(jnp.int32, (128, 128), 1) // 32
    ).astype(F32).astype(BF16)

    def place(x, at):
        line_ranks = jnp.broadcast_to(limits[pl.ds(x + 8, 1), :], (ny, 128))
        picks[pl.ds(pl.multiple_of(at * ny, ny), ny), :] = jnp.where(own, line_ranks, 0.0).astype(BF16)

    def place_own(x, _):
        place(x, x)
        return 0

    lax.fori_loop(0, nx, place_own, 0, unroll=4)
    place(-1, nx)
    place(nx, nx + 1)

    def fill_mask(i, _):
        mask[flat(i), :] = jnp.where(level(rows) < dot(picks[flat(i), :], spread), 1.0, 0.0)
        return 0

    lax.fori_loop(0, chunks, fill_mask, 0)
    mask[lines : lines + 2 * ny, :] = jnp.where(level(2 * ny) < dot(picks[lines : lines + 2 * ny, :], spread), 1.0, 0.0)
    edge_mask[0:ny, :] = jnp.where(segments(ny) == 1, mask[0:ny, :], 0.0)
    edge_mask[ny : 2 * ny, :] = jnp.where(segments(ny) == 0, mask[lines - ny : lines, :], 0.0)
    edge_mask[2 * ny : 2 * ny + nx, :] = jnp.where(segments(nx) == 2, mask[pl.ds(ny - 1, nx, stride=ny), :], 0.0)
    edge_mask[2 * ny + nx : edge, :] = jnp.where(segments(nx) == 3, mask[pl.ds(0, nx, stride=ny), :], 0.0)

    diagonal(u0, inner)
    couple(0, u0, inner)
    finish_field(0, u0)

    operate(1, u0, v0, 0, lambda x, here, value, carry: carry, coefs_and_send(1))

    diagonal(u1, inner)

    def early(x, total, carry):
        have = u0[cells(x), :]
        return (
            carry[0] + fold(have * b[x]), carry[1] + fold(have * v0[x]),
            carry[2] + fold(total * b[x]), carry[3] + fold(total * v0[x]),
        )

    bu0, u0v0, bu1, v0u1 = couple(1, u1, inner, (zero, zero, zero, zero), early)
    more = finish_field(1, u1)
    pieces = (
        (more[:ny], lambda k: fields[k][0]),
        (more[ny : 2 * ny], lambda k: fields[k][nx - 1]),
        (more[2 * ny : 2 * ny + nx], lambda k: raw_send[k, 1]),
        (more[2 * ny + nx :], lambda k: raw_send[k, 0]),
    )
    for piece, line_of in pieces:
        bu1 = bu1 + fold(piece * line_of(0))
        v0u1 = v0u1 + fold(piece * line_of(1))

    u1v1 = operate(
        2, u1, v1, zero, lambda x, here, value, carry: carry + fold(here * value), lambda turn, i: None
    )

    def row_of(value):
        value = value[:, :128] + value[:, 128:]
        return jnp.sum(value, axis=0, keepdims=True)

    partial = jnp.concatenate(
        [row_of(s) for s in (bu0, u0v0, bu1, v0u1, u1v1)] + [jnp.zeros((3, 128), F32)], axis=0
    )
    part[0] = partial
    got_y[gy] = partial
    along_y = [
        pltpu.make_async_remote_copy(
            src_ref=part.at[0], dst_ref=got_y.at[gy], send_sem=rsend_sem.at[0, k], recv_sem=rrecv_sem.at[0, k],
            device_id=(gx, lax.rem(gy + k, ndy)), device_id_type=MESH,
        )
        for k in range(1, ndy)
    ]
    for copy in along_y:
        copy.start()

    def last_send(turn, _):
        coefs_and_send(2)(turn, chunk(turn))
        return 0

    lax.fori_loop(0, chunks, last_send, 0)
    diagonal(u2, flat)
    couple(2, u2, flat)
    for copy in along_y:
        copy.wait()
    partial = jnp.sum(got_y[...], axis=0)
    part[1] = partial
    got_x[gx] = partial
    along_x = [
        pltpu.make_async_remote_copy(
            src_ref=part.at[1], dst_ref=got_x.at[gx], send_sem=rsend_sem.at[1, k], recv_sem=rrecv_sem.at[1, k],
            device_id=(lax.rem(gx + k, ndx), gy), device_id_type=MESH,
        )
        for k in range(1, ndx)
    ]
    for copy in along_x:
        copy.start()
    for copy in all_copies(2):
        copy.wait_recv()
    fix_own(2)
    value = fsplit[0:edge, :]
    more = dot(jnp.concatenate([value, value[:, :128]], axis=1), wd[...])
    uy[2 * nx : 4 * nx, :] = more[2 * ny :]
    u2[0:ny, :] = u2[0:ny, :] + more[:ny]
    u2[lines - ny : lines, :] = u2[lines - ny : lines, :] + more[ny : 2 * ny]
    add_ends(u2, 0, 3 * nx, 2 * nx)
    for k in range(3):
        for copy in all_copies(k):
            copy.wait_send()
    for copy in along_x:
        copy.wait()
    total = jnp.sum(jnp.sum(got_x[...], axis=0), axis=1, keepdims=True)
    s = [total[k : k + 1, :] for k in range(5)]

    alpha0 = s[S_BU0] / s[S_U0V0]
    rz1 = s[S_BU0] - alpha0 * (s[S_U0V0] + s[S_BU1]) + alpha0 * (alpha0 * s[S_V0U1])
    grow = 1.0 + rz1 / s[S_BU0]
    curve = grow * (grow * s[S_U0V0] - 2.0 * (alpha0 * s[S_V0U1])) + alpha0 * (alpha0 * s[S_U1V1])
    alpha1 = rz1 / curve
    on0 = alpha0 + alpha1 * grow
    on1 = -(alpha1 * alpha0)
    scale[0] = jnp.broadcast_to(on0, (8, 128))
    scale[1] = jnp.broadcast_to(on1, (8, 128))


def combine(b, u0, u1, u2, v0, v1, scale, x_any, gap_any, z_any, x_out, gap_out, z_out, sem):
    nx, ny, nz = x_out.shape
    step = 4
    on0, on1 = (jnp.concatenate([jnp.concatenate([scale[k]] * 2, axis=1)] * (ny // 8), axis=0) for k in (0, 1))

    def copies(i):
        here = pl.ds(pl.multiple_of(i * step, step), step)
        return [
            pltpu.make_async_copy(out.at[here], out_any.at[here], sem.at[n, i])
            for n, (out, out_any) in enumerate(((x_out, x_any), (z_out, z_any), (gap_out, gap_any)))
        ]

    def body(i, _):
        for j in range(step):
            x = i * step + j
            at = pl.ds(pl.multiple_of((x + 1) * ny, ny), ny)
            f0, f1 = u0[at, :], u1[at, :]
            x_out[x] = on0 * f0 + on1 * f1
            z_out[x] = f0 - on0 * f1 - on1 * u2[pl.ds(pl.multiple_of(x * ny, ny), ny), :]
            gap_out[x] = b[x] - on0 * v0[x] - on1 * v1[x]
        for copy in copies(i):
            copy.start()
        return 0

    lax.fori_loop(0, nx // step, body, 0)

    def finish(i, _):
        for copy in copies(i):
            copy.wait()
        return 0

    lax.fori_loop(0, nx // step, finish, 0)


def per_device(devs, right_side, block_inverse, basis_left, basis_right, ranks):
    nx, ny, nz = right_side.shape
    ndx, ndy = devs
    lines = nx * ny
    padded = lines + 2 * ny
    edge = 2 * (nx + ny)
    block = jax.ShapeDtypeStruct(right_side.shape, F32)
    framed = jax.ShapeDtypeStruct((padded, nz), F32)
    arrays = (right_side, block_inverse, basis_left, basis_right, ranks)
    fields = pl.pallas_call(
        functools.partial(kernel, devs),
        out_shape=(
            block, framed, framed, jax.ShapeDtypeStruct((lines, nz), F32), block, block,
            jax.ShapeDtypeStruct((2, 8, 128), F32),
        ),
        in_specs=[pl.BlockSpec(memory_space=pltpu.HBM)] * 5,
        out_specs=[pl.BlockSpec(memory_space=pltpu.VMEM)] * 7,
        scratch_shapes=[
            pltpu.VMEM((nz, nz), F32),
            pltpu.VMEM((4, 32, nz), F32),
            pltpu.VMEM((2, 3, nx + 16, 128), jnp.int32),
            pltpu.VMEM((nx + 16, 128), F32),
            pltpu.VMEM((lines + 2 * ny, 128), BF16),
            pltpu.VMEM((3 * nz, nz), BF16),
            pltpu.VMEM((2 * nz, 256), BF16),
            pltpu.VMEM((384, nz), BF16),
            pltpu.VMEM((lines + edge, 128), F32),
            pltpu.VMEM((edge, 128), F32),
            pltpu.VMEM((lines, 2 * nz), BF16),
            pltpu.VMEM((16 * ny, 256), BF16),
            pltpu.VMEM((2 * edge, 256), BF16),
            pltpu.VMEM((3, padded, 128), F32),
            pltpu.VMEM((3, edge, 128), F32),
            pltpu.VMEM((3, edge, 128), F32),
            pltpu.VMEM((2, 2, nx, nz), F32),
            pltpu.VMEM((2, edge, nz), F32),
            pltpu.VMEM((2, 4, 8, 128), F32),
            pltpu.VMEM((2, 4, 8, 128), F32),
            pltpu.VMEM((4 * nx, nz), F32),
            pltpu.VMEM((2, 8, 128), F32),
            pltpu.VMEM((ndy, 8, 128), F32),
            pltpu.VMEM((ndx, 8, 128), F32),
            pltpu.SemaphoreType.DMA((24,)),
            pltpu.SemaphoreType.DMA((3, 2, 2)),
            pltpu.SemaphoreType.DMA((3, 2, 2)),
            pltpu.SemaphoreType.DMA((3, 2, 2, nx // 16)),
            pltpu.SemaphoreType.DMA((3, 2, 2, nx // 16)),
            pltpu.SemaphoreType.DMA((2, 4)),
            pltpu.SemaphoreType.DMA((2, 4)),
            pltpu.SemaphoreType.DMA((2, ndy)),
            pltpu.SemaphoreType.DMA((2, ndy)),
        ],
        compiler_params=pltpu.CompilerParams(
            collective_id=0, has_side_effects=True, vmem_limit_bytes=32 * 1024 * 1024
        ),
    )(*(pltpu.with_memory_space_constraint(array, pltpu.HBM) for array in arrays))
    return pl.pallas_call(
        combine,
        out_shape=(block, block, block),
        in_specs=[pl.BlockSpec(memory_space=pltpu.VMEM)] * 7,
        out_specs=[pl.BlockSpec(memory_space=pltpu.HBM)] * 3,
        scratch_shapes=[pltpu.VMEM((nx, ny, nz), F32)] * 3 + [pltpu.SemaphoreType.DMA((3, nx // 4))],
        compiler_params=pltpu.CompilerParams(vmem_limit_bytes=32 * 1024 * 1024),
    )(*fields)


def solution(mesh):
    devs = (mesh.shape["gx"], mesh.shape["gy"])
    return jax.shard_map(
        functools.partial(per_device, devs),
        mesh=mesh,
        in_specs=(P("gx", "gy", None), P(), P(), P(), P()),
        out_specs=(P("gx", "gy", None),) * 3,
        check_vma=False,
    )
```
